512 devices in a mesh: ell: 16 (over y, z_lo), blk: 32 (over x, z_hi, core).
Axes of the slice: x: 4, y: 4, z: 16 (z_hi: 4, z_lo: 4; z = z_hi * 4 + z_lo), core: 2. Of those that a mesh axis runs over, the one named last changes fastest.
Arguments:
- wigner: bfloat16 [32, 17, 2162688], P(None, None, ('ell', 'blk')), may hold values from -6 to 6
- sky_alm: float32 [2, 2162688], P(None, ('ell', 'blk')), may hold values from -0.03125 to 0.03125
- beam_blm: float32 [2, 17, 2048], replicated, may hold values from -4.25 to 4.25
- slot_col: int32 [2162688], P(('ell', 'blk')), may hold values from -1 to 63, as said below
- slot_ell: int32 [2162688], P(('ell', 'blk')), may hold values from 0 to 2047, as said below
- order_of_column: int32 [2048], replicated, may hold values from 0 to 2047, as said below
Outputs:
- conv_cube: float32 [32, 32, 4096], P('ell', 'blk')
The draws below stay inside these ranges and needn't reach their ends.
Inputs may be any that keep to these rules, and one draw needn't show every extreme that they name: `slot_col`: slot block b (slots b * 4224 to b * 4224 + 4223) belongs to ell index b // 32 and blk index b % 32; at most 4098 slots of a block are live, and some blocks have exactly that many. `slot_ell`: every pair (l, m) with m <= l < 2048 stands in exactly one live slot; within a blk group, higher ell indices hold degrees no lower than those of lower ell indices. `order_of_column`: A permutation of 0 to 2047; every blk group's orders hold the same number of pairs.
All inputs are finite; a program needn't handle non-finite values.
Results may differ from the reference program's by a relative error of at most 0.0029.
Values sent between devices are 32-bit elements; how exact they have to be, the bound alone decides.
A program may use at most 64 MiB of HBM per device.

```python
import math
import jax
import jax.numpy as jnp
from jax import lax

L = 2048
K = 17
NPSI = 32
THETA = 32
NPHI = 4096
M_DEV = 64
LIVE_MOST = 4098
SLOT_DEV = 4224
SLOTS = 2162688
N_ELL = 16
N_BLK = 32


def pair_tables(key):
    half = L // 2
    fold = L // (2 * N_BLK)
    blocks = N_ELL * N_BLK
    cols = L // N_BLK
    order = jax.random.permutation(jax.random.fold_in(key, 101), half)
    lower = order.reshape(N_BLK, fold)
    grouped = jnp.concatenate([lower, L - 1 - lower], axis=1).astype(jnp.int32)
    col_keys = jax.random.split(jax.random.fold_in(key, 102), N_BLK)
    col_perm = jax.vmap(lambda inner_key: jax.random.permutation(inner_key, cols))(col_keys)
    order_table = jnp.take_along_axis(grouped, col_perm.astype(jnp.int32), axis=1)
    degrees = jnp.arange(L, dtype=jnp.int32)
    valid = order_table[:, None, :] <= degrees[None, :, None]
    flat_valid = valid.reshape(N_BLK, L * cols)
    position = jnp.cumsum(flat_valid.astype(jnp.int32), axis=1) - 1
    ell_index = position // LIVE_MOST
    offset = jnp.clip(position % LIVE_MOST, 0, SLOT_DEV - 1)
    group_index = jnp.arange(N_BLK, dtype=jnp.int32)[:, None]
    block = jnp.clip(ell_index * N_BLK + group_index, 0, blocks - 1)
    shuffle_keys = jax.random.split(jax.random.fold_in(key, 103), blocks)
    shuffles = jax.vmap(lambda inner_key: jax.random.permutation(inner_key, SLOT_DEV))(shuffle_keys).astype(jnp.int32)
    slot = block * SLOT_DEV + shuffles[block, offset]
    target = jnp.where(flat_valid, slot, blocks * SLOT_DEV).reshape(-1)
    col_values = jnp.broadcast_to(jnp.arange(cols, dtype=jnp.int32)[None, None, :], (N_BLK, L, cols)).reshape(-1)
    ell_values = jnp.broadcast_to(degrees[None, :, None], (N_BLK, L, cols)).reshape(-1)
    slot_col = jnp.full((blocks * SLOT_DEV,), -1, jnp.int32).at[target].set(col_values, mode='drop')
    slot_ell = jnp.zeros((blocks * SLOT_DEV,), jnp.int32).at[target].set(ell_values, mode='drop')
    return (order_table.reshape(L), slot_col, slot_ell)


def draw_order_of_column(key, part):
    return pair_tables(key)[0]


def draw_slot_col(key, part):
    return pair_tables(key)[1]


def draw_slot_ell(key, part):
    return pair_tables(key)[2]


def draw_beam_blm(key, part):
    degrees = jnp.arange(L, dtype=jnp.float32)
    scale = (2.0 * (degrees + 1.0)) ** (-0.5)
    base = jnp.clip(jax.random.normal(key, (2, K, L), jnp.float32), -6.0, 6.0)
    return (base * scale[None, None, :]).astype(jnp.float32)


def level_of(key, shape, pieces, low, top_value):
    def one(dim, blocks):
        draws = jax.random.uniform(jax.random.fold_in(jax.random.fold_in(key, 6), dim), (blocks,), jnp.float32, low / len(pieces), top_value / len(pieces))
        return jnp.repeat(jnp.exp(draws), shape[dim] // blocks).reshape((-1,) + (1,) * (len(shape) - dim - 1))

    gain = one(*pieces[0])
    for cut in pieces[1:]:
        gain = gain * one(*cut)
    return gain


def scatter_about(rng, shape, deviation, reach, shards=(), held_as=jnp.bfloat16):
    array = jax.random.normal(rng, shape, jnp.float32) * deviation
    if len(shards) > 0:
        array = level_of(rng, shape, shards, -0.22, 0.18) * array
    return jnp.clip(array, min=-reach, max=reach).astype(held_as)


def setup_inputs(seed: int = 0) -> dict:
    key_of = jax.random.split(jax.random.key(seed), 7)
    wigner = scatter_about(key_of[0], (THETA, K, SLOTS), 1.0, 6.0, ((2, 512),))
    sky_alm = scatter_about(key_of[1], (2, SLOTS), (L * K) ** -0.5, 0.03125, ((1, 512),), jnp.float32)
    beam_blm = draw_beam_blm(jax.random.fold_in(key_of[6], 71), 0)
    slot_col = draw_slot_col(jax.random.fold_in(key_of[6], 71), 0)
    slot_ell = draw_slot_ell(jax.random.fold_in(key_of[6], 71), 0)
    order_of_column = draw_order_of_column(jax.random.fold_in(key_of[6], 71), 0)
    return dict(wigner=wigner, sky_alm=sky_alm, beam_blm=beam_blm, slot_col=slot_col, slot_ell=slot_ell, order_of_column=order_of_column)


def phase_table(rows, cols, period):
    product = (jnp.arange(rows, dtype=jnp.int32)[:, None] * jnp.arange(cols, dtype=jnp.int32)[None, :]) % period
    angle = product.astype(jnp.float32) * (2.0 * math.pi / period)
    return jnp.cos(angle), jnp.sin(angle)


def psi_table(order_count, samples):
    cosines, sine_terms = phase_table(order_count, samples, samples)
    real_row = jnp.stack([cosines, sine_terms], axis=1)
    imag_row = jnp.stack([-sine_terms, cosines], axis=1)
    return jnp.stack([real_row, imag_row], axis=0)


def reference(wigner, sky_alm, beam_blm, slot_col, slot_ell, order_of_column):
    block_count = SLOTS // SLOT_DEV

    def accumulate(running, block_index):
        first_slot = block_index * SLOT_DEV
        wig_rows = lax.dynamic_slice_in_dim(wigner, first_slot, SLOT_DEV, 2).astype(jnp.float32)
        alm_part = lax.dynamic_slice_in_dim(sky_alm, first_slot, SLOT_DEV, 1)
        columns = lax.dynamic_slice_in_dim(slot_col, first_slot, SLOT_DEV, 0)
        degrees = lax.dynamic_slice_in_dim(slot_ell, first_slot, SLOT_DEV, 0)
        beam_slots = jnp.take(beam_blm, degrees, axis=2)
        coeffs = jnp.stack([alm_part[0] * beam_slots[0] - alm_part[1] * beam_slots[1],
                            alm_part[0] * beam_slots[1] + alm_part[1] * beam_slots[0]])
        values = (wig_rows[:, None] * coeffs[None]).astype(jnp.bfloat16)
        values = lax.optimization_barrier(values).astype(jnp.float32)
        group = (block_index % N_BLK).astype(jnp.int32)
        global_col = group * M_DEV + jnp.maximum(columns, 0)
        orders = jnp.where(columns >= 0, jnp.take(order_of_column, global_col), L).astype(jnp.int32)
        flat = values.reshape(THETA * 2 * K, SLOT_DEV).T
        return running + jax.ops.segment_sum(flat, orders, num_segments=L + 1)[:L], None

    totals, _ = lax.scan(accumulate, jnp.zeros((L, THETA * 2 * K), jnp.float32),
                         jnp.arange(block_count, dtype=jnp.int32))
    harmonic = totals.T.reshape(THETA, 2, K, L)
    psi_field = jnp.einsum("trkc,rksp->tspc", harmonic, psi_table(K, NPSI), precision=lax.Precision.HIGHEST)
    complex_field = psi_field[:, 0] + 1j * psi_field[:, 1]
    padded = jnp.pad(complex_field, ((0, 0), (0, 0), (0, NPHI - L)))
    return (jnp.real(jnp.fft.ifft(padded, axis=-1)) * NPHI).astype(jnp.float32)
```

```python
import math

import jax
import jax.numpy as jnp
import numpy as np
from jax import lax
from jax.experimental import pallas as pl
from jax.experimental.pallas import tpu as pltpu
from jax.sharding import PartitionSpec as P

F32, BF16, I32 = jnp.float32, jnp.bfloat16, jnp.int32
MESH = pl.DeviceIdType.MESH
K, T, C = 17, 32, 64
BLKS = 32

def build_table(beam, table):
    rows = jnp.concatenate([beam[:, 0, :], beam[:, 1, :], jnp.zeros((6, 2048), F32)], axis=0)
    high = rows.astype(BF16)
    low = (rows - high.astype(F32)).astype(BF16)
    for h in range(16):
        span = slice(h * 128, h * 128 + 128)
        table[h, :, 0:128] = high[:, span]
        table[h, :, 128:256] = low[:, span]


def gather_block(table, ell, sky, coef, row, cols):
    n = 128 * cols
    degree = jnp.concatenate([ell[pl.ds(row + c, 1), :] for c in range(cols)], axis=1)
    low = degree & 127
    high = degree >> 7
    hot = (lax.broadcasted_iota(I32, (128, n), 0) == low).astype(F32).astype(BF16)
    hot = jnp.concatenate([hot, hot], axis=0)
    lhs = table[...].reshape(16 * 40, 256)
    picked = jnp.dot(lhs, hot, preferred_element_type=F32)
    total = jnp.zeros((40, n), F32)
    for h in range(16):
        total = jnp.where(high == h, picked[h * 40 : h * 40 + 40], total)
    br, bi = total[0:17], total[17:34]
    start = pl.multiple_of(row * 128, 128)
    s0 = sky[0:1, pl.ds(start, n)]
    s1 = sky[1:2, pl.ds(start, n)]
    coef[0, 0:17, pl.ds(start, n)] = s0 * br - s1 * bi
    coef[1, 0:17, pl.ds(start, n)] = s0 * bi + s1 * br


def add_block(wig, coef, col, acc, row, cols):
    lhs = []
    rhs = []
    zero = jnp.zeros((64, 128), BF16)
    for c in range(cols):
        start = pl.multiple_of((row + c) * 128, 128)
        span = pl.ds(start, 128)
        re, im = [], []
        for k in range(K):
            w = wig[k, :, span].astype(F32)
            re.append((w * coef[0, pl.ds(k, 1), span]).astype(BF16))
            im.append((w * coef[1, pl.ds(k, 1), span]).astype(BF16))
        lhs += [jnp.concatenate(re, axis=0), jnp.concatenate(im, axis=0)]
        hot = (lax.broadcasted_iota(I32, (64, 128), 0) == col[pl.ds(row + c, 1), :]).astype(F32).astype(BF16)
        rhs += [jnp.concatenate([hot, zero], axis=0), jnp.concatenate([zero, hot], axis=0)]
    left = jnp.concatenate(lhs, axis=1)
    right = jnp.concatenate(rhs, axis=1)
    part = lax.dot_general(left, right, (((1,), (1,)), ((), ())), preferred_element_type=F32)
    acc[...] += part.reshape(K, T, 128)


def compute(wig, sky, beam, col, ell, table, coef, acc):
    build_table(beam, table)

    def gather_step(i, _):
        gather_block(table, ell, sky, coef, i * 2, 2)
        return 0

    lax.fori_loop(0, 16, gather_step, 0)
    gather_block(table, ell, sky, coef, 32, 1)
    acc[...] = jnp.zeros((K, T, 128), F32)

    def add_step(i, _):
        add_block(wig, coef, col, acc, i * 3, 3)
        return 0

    lax.fori_loop(0, 11, add_step, 0)


def constants():
    out = np.zeros((448, 128), np.float64)
    for p in range(32):
        for tt in range(2):
            for k in range(K):
                at = tt * 16 + k if k < 16 else 32 + tt
                angle = 2.0 * math.pi * (k * p % 32) / 32
                out[p * 2 + tt, at] = math.cos(angle)
                out[64 + p * 2 + tt, at] = math.sin(angle)
    n = np.arange(64)
    angle = 2.0 * math.pi * (np.outer(n, np.arange(32)) % 64) / 64
    out[128:192, :32] = np.cos(angle)
    out[192:256, :32] = np.sin(angle)
    angle = 2.0 * math.pi * np.outer(n, n) / 4096
    out[256:320] = np.concatenate([np.cos(angle), np.cos(angle)], 1)
    out[320:384] = np.concatenate([-np.sin(angle), np.sin(angle)], 1)
    w = np.concatenate([n[0::2], n[1::2]])
    angle = 2.0 * math.pi * (np.outer(w, n) % 64) / 64
    out[384:448] = np.concatenate([np.cos(angle), -np.sin(angle)], 1)
    return out.astype(np.float32)


def dot_exact(a, b, contract=((1,), (0,))):
    return lax.dot_general(
        a, b, (contract, ((), ())), precision=lax.Precision.HIGHEST, preferred_element_type=F32
    )


def rotated(x):
    return pltpu.roll(x, 64, 1)


def turned(both, sign):
    half = both.shape[0] // 2
    return both[:half] + sign * rotated(both[half:])


def kernel(
    wig_hbm, sky_hbm, beam_hbm, col_hbm, ell_hbm, ooc_hbm, const_hbm,
    out_ref,
    wig, sky, beam, col, ell, ooc, const,
    table, coef, acc, from_y, hy, to_z, from_z, ps, got, key, hot_low, grid,
    in_sem, y_send, y_recv, z_send, z_recv, b_send, b_recv,
):
    e = lax.axis_index("ell")
    b = lax.axis_index("blk")
    y, z = e // 4, e % 4
    x, zh, core = b // 8, (b // 2) % 4, b % 2

    def y_peer(d):
        return (lax.rem(y + d, 4) * 4 + z, b)

    def z_peer(d):
        return (y * 4 + lax.rem(z + d, 4), b)

    def b_peer(d):
        return (e, lax.rem(b + d, BLKS))

    loads = [
        pltpu.make_async_copy(src, dst, in_sem.at[i])
        for i, (src, dst) in enumerate(
            [
                (beam_hbm, beam), (ell_hbm, ell), (sky_hbm, sky), (wig_hbm, wig),
                (col_hbm, col), (const_hbm, const), (ooc_hbm, ooc),
            ]
        )
    ]
    for load in loads:
        load.start()
    barrier = pltpu.get_barrier_semaphore()
    peers = [y_peer(d) for d in range(1, 4)] + [z_peer(d) for d in range(1, 4)]
    peers += [b_peer(d) for d in range(1, BLKS)]
    for peer in peers:
        pl.semaphore_signal(barrier, inc=1, device_id=peer, device_id_type=MESH)
    for load in loads:
        load.wait()

    compute(wig, sky, beam, col, ell, table, coef, acc)

    pl.semaphore_wait(barrier, len(peers))

    def y_copy(d):
        there = pl.multiple_of(lax.rem(y + d, 4) * 8, 8)
        return pltpu.make_async_remote_copy(
            src_ref=acc.at[:, pl.ds(there, 8), :], dst_ref=from_y.at[d - 1],
            send_sem=y_send.at[d - 1], recv_sem=y_recv.at[d - 1],
            device_id=y_peer(d), device_id_type=MESH,
        )

    y_copies = [y_copy(d) for d in (2, 1, 3)]
    for copy in y_copies:
        copy.start()

    lane = lax.broadcasted_iota(I32, (16, 128), 1)
    order = ooc[...]
    swapped = rotated(order)
    even = jnp.where(lane < 64, order, swapped)
    odd = jnp.where(lane < 64, swapped, order)
    side = jnp.where(lane < 64, 0, 64)
    key[0] = (even & 63) + side
    key[1] = (odd & 63) + side
    key[2] = even >> 6
    key[3] = odd >> 6
    rows = lax.broadcasted_iota(I32, (128, 128), 0)

    def low_step(a, _):
        hot_low[a, :, 0:128] = (rows == key[0, pl.ds(a, 1), :]).astype(F32).astype(BF16)
        hot_low[a, :, 128:256] = (rows == key[1, pl.ds(a, 1), :]).astype(F32).astype(BF16)
        return 0

    lax.fori_loop(0, 16, low_step, 0)
    grid[...] = jnp.zeros((64, 128), F32)
    to_z[:, 32:40, :] = jnp.zeros((4, 8, 128), F32)

    for copy in y_copies:
        copy.wait_recv()
    mine = pl.multiple_of(y * 8, 8)
    total = acc[:, pl.ds(mine, 8), :] + from_y[0] + from_y[1] + from_y[2]
    hy[...] = total.reshape(K * 8, 128)
    for d in range(4):
        for tt in range(2):
            at = 2 * d + tt
            to_z[d, tt * 16 : tt * 16 + 8, :] = hy[pl.ds(at, 8, stride=8), :]
            to_z[d, tt * 16 + 8 : tt * 16 + 16, :] = hy[pl.ds(64 + at, 8, stride=8), :]
            to_z[d, 32 + tt : 33 + tt, :] = hy[128 + at : 129 + at, :]

    def z_copy(d):
        return pltpu.make_async_remote_copy(
            src_ref=to_z.at[lax.rem(z + d, 4)], dst_ref=from_z.at[d - 1],
            send_sem=z_send.at[d - 1], recv_sem=z_recv.at[d - 1],
            device_id=z_peer(d), device_id_type=MESH,
        )

    z_copies = [z_copy(d) for d in (2, 1, 3)]
    for copy in z_copies:
        copy.start()
    for copy in z_copies:
        copy.wait_recv()
    summed = to_z[z] + from_z[0] + from_z[1] + from_z[2]
    lanes = lax.broadcasted_iota(I32, (1, 128), 1)
    sign = jnp.where(lanes < 64, -1.0, 1.0).astype(F32)
    psi = turned(dot_exact(const[0:128, 0:40], summed), sign)
    for p in range(BLKS):
        ps[p] = psi[2 * p : 2 * p + 2]

    def b_copy(d):
        there = lax.rem(b + d, BLKS)
        return pltpu.make_async_remote_copy(
            src_ref=ps.at[there], dst_ref=got.at[b],
            send_sem=b_send.at[d], recv_sem=b_recv.at[b],
            device_id=b_peer(d), device_id_type=MESH,
        )

    b_copies = [b_copy(d) for d in range(1, BLKS)]
    for copy in b_copies:
        copy.start()
    got[b] = ps[b]

    highs = lax.broadcasted_iota(I32, (32, 128), 0)
    steps = sorted(
        ((dx, dz) for dx in range(4) for dz in range(4)),
        key=lambda s: min(s[0], 4 - s[0]) + 4 * min(s[1], 4 - s[1]),
    )
    for dx, dz in steps:
        chip = lax.rem(x + dx, 4) * 4 + lax.rem(zh + dz, 4)
        for c in range(2):
            source = chip * 2 + c
            arrival = pltpu.make_async_remote_copy(
                src_ref=ps.at[0], dst_ref=got.at[source],
                send_sem=b_send.at[0], recv_sem=b_recv.at[source],
                device_id=(e, source), device_id_type=MESH,
            )
            if (dx, dz) == (0, 0):
                @pl.when(core != c)
                def _():
                    arrival.wait_recv()
            else:
                arrival.wait_recv()
        parts = []
        for c in range(2):
            value = got[chip * 2 + c]
            here = highs == key[2 + c, pl.ds(chip, 1), :]
            spread = jnp.concatenate(
                [jnp.where(here, value[tt : tt + 1, :], 0.0) for tt in range(2)], axis=0
            )
            high = spread.astype(BF16)
            parts.append(jnp.concatenate([high, (spread - high.astype(F32)).astype(BF16)], axis=0))
        placed = lax.dot_general(
            jnp.concatenate(parts, axis=1), hot_low[chip], (((1,), (1,)), ((), ())),
            preferred_element_type=F32,
        )
        grid[...] += placed[0:64] + placed[64:128]

    results = []
    for tt in range(2):
        first = turned(dot_exact(const[128:256, 0:32], grid[tt * 32 : tt * 32 + 32, :]), sign)
        results.append(first * const[256:320, :] + rotated(first) * const[320:384, :])
    last = dot_exact(const[384:448, :], jnp.concatenate(results, axis=0), ((1,), (1,)))
    low, upp = last[0:32], last[32:64]
    left = lax.broadcasted_iota(I32, (32, 128), 1) < 64
    out_ref[0] = jnp.where(left, low, rotated(upp))
    out_ref[1] = jnp.where(left, rotated(low), upp)
    for copy in y_copies + z_copies + b_copies:
        copy.wait_send()


def on_device(wigner, sky_alm, beam_blm, slot_col, slot_ell, order_of_column):
    q = wigner.shape[2]
    any_space = pl.BlockSpec(memory_space=pl.ANY)
    dma = pltpu.SemaphoreType.DMA
    out = pl.pallas_call(
        kernel,
        out_shape=jax.ShapeDtypeStruct((2, 32, 128), F32),
        in_specs=[any_space] * 7,
        out_specs=pl.BlockSpec(memory_space=pltpu.VMEM),
        scratch_shapes=[
            pltpu.VMEM((K, T, q), BF16),
            pltpu.VMEM((2, q), F32),
            pltpu.VMEM((K, 2, 2048), F32),
            pltpu.VMEM((q // 128, 128), I32),
            pltpu.VMEM((q // 128, 128), I32),
            pltpu.VMEM((16, 128), I32),
            pltpu.VMEM((448, 128), F32),
            pltpu.VMEM((16, 40, 256), BF16),
            pltpu.VMEM((2, 24, q), F32),
            pltpu.VMEM((K, T, 128), F32),
            pltpu.VMEM((3, K, 8, 128), F32),
            pltpu.VMEM((K * 8, 128), F32),
            pltpu.VMEM((4, 40, 128), F32),
            pltpu.VMEM((3, 40, 128), F32),
            pltpu.VMEM((BLKS, 2, 128), F32),
            pltpu.VMEM((BLKS, 2, 128), F32),
            pltpu.VMEM((4, 16, 128), I32),
            pltpu.VMEM((16, 128, 256), BF16),
            pltpu.VMEM((64, 128), F32),
            dma((7,)),
            dma((3,)), dma((3,)), dma((3,)), dma((3,)), dma((BLKS,)), dma((BLKS,)),
        ],
        compiler_params=pltpu.CompilerParams(
            collective_id=0, has_side_effects=True, vmem_limit_bytes=60000 * 1024
        ),
    )(
        jnp.transpose(wigner, (1, 0, 2)),
        sky_alm,
        jnp.transpose(beam_blm, (1, 0, 2)),
        slot_col.reshape(q // 128, 128),
        slot_ell.reshape(q // 128, 128),
        order_of_column.reshape(16, 128),
        jnp.asarray(constants()),
    )
    return out.reshape(2, 1, 4096)


def solution(mesh):
    return jax.shard_map(
        on_device,
        mesh=mesh,
        in_specs=(
            P(None, None, ("ell", "blk")),
            P(None, ("ell", "blk")),
            P(),
            P(("ell", "blk")),
            P(("ell", "blk")),
            P(),
        ),
        out_specs=P("ell", "blk", None),
        check_vma=False,
    )
```

```python
import math

import jax
import jax.numpy as jnp
import numpy as np
from jax import lax
from jax.experimental import pallas as pl
from jax.experimental.pallas import tpu as pltpu
from jax.sharding import PartitionSpec as P

F32, BF16, I32 = jnp.float32, jnp.bfloat16, jnp.int32
MESH = pl.DeviceIdType.MESH
K, T, C = 17, 32, 64
BLKS = 32

def build_table(beam, table):
    rows = jnp.concatenate([beam[:, 0, :], beam[:, 1, :], jnp.zeros((6, 2048), F32)], axis=0)
    high = rows.astype(BF16)
    low = (rows - high.astype(F32)).astype(BF16)
    for h in range(16):
        span = slice(h * 128, h * 128 + 128)
        table[h, :, 0:128] = high[:, span]
        table[h, :, 128:256] = low[:, span]


def gather_block(base, table, ell, sky, coef, row, cols):
    n = 128 * cols
    degree = jnp.concatenate([ell[pl.ds(row + c, 1), :] for c in range(cols)], axis=1)
    low = degree & 127
    high = (degree >> 7) - base
    hot = (lax.broadcasted_iota(I32, (128, n), 0) == low).astype(F32).astype(BF16)
    hot = jnp.concatenate([hot, hot], axis=0)
    lhs = table[pl.ds(base, 10)].reshape(10 * 40, 256)
    picked = jnp.dot(lhs, hot, preferred_element_type=F32)
    total = jnp.zeros((40, n), F32)
    for h in range(10):
        total = jnp.where(high == h, picked[h * 40 : h * 40 + 40], total)
    br, bi = total[0:17], total[17:34]
    start = pl.multiple_of(row * 128, 128)
    s0 = sky[0:1, pl.ds(start, n)]
    s1 = sky[1:2, pl.ds(start, n)]
    coef[0, 0:17, pl.ds(start, n)] = s0 * br - s1 * bi
    coef[1, 0:17, pl.ds(start, n)] = s0 * bi + s1 * br


def add_block(wig, coef, col, acc, row, cols):
    lhs = []
    rhs = []
    zero = jnp.zeros((64, 128), BF16)
    for c in range(cols):
        start = pl.multiple_of((row + c) * 128, 128)
        span = pl.ds(start, 128)
        re, im = [], []
        for k in range(K):
            w = wig[k, :, span].astype(F32)
            re.append((w * coef[0, pl.ds(k, 1), span]).astype(BF16))
            im.append((w * coef[1, pl.ds(k, 1), span]).astype(BF16))
        lhs += [jnp.concatenate(re, axis=0), jnp.concatenate(im, axis=0)]
        hot = (lax.broadcasted_iota(I32, (64, 128), 0) == col[pl.ds(row + c, 1), :]).astype(F32).astype(BF16)
        rhs += [jnp.concatenate([hot, zero], axis=0), jnp.concatenate([zero, hot], axis=0)]
    left = jnp.concatenate(lhs, axis=1)
    right = jnp.concatenate(rhs, axis=1)
    part = lax.dot_general(left, right, (((1,), (1,)), ((), ())), preferred_element_type=F32)
    acc[...] += part.reshape(K, T, 128)


def gather_all(sky, beam, col, ell, table, coef):
    build_table(beam, table)
    base = jnp.minimum(jnp.min(jnp.where(col[...] >= 0, ell[...], 2047)) >> 7, 6)
    gather_block(base, table, ell, sky, coef, 0, ell.shape[0])


def add_all(wig, col, coef, acc):
    acc[...] = jnp.zeros((K, T, 128), F32)
    add_block(wig, coef, col, acc, 0, col.shape[0])


def constants():
    out = np.zeros((448, 128), np.float64)
    for p in range(32):
        for tt in range(2):
            for k in range(K):
                at = tt * 16 + k if k < 16 else 32 + tt
                angle = 2.0 * math.pi * (k * p % 32) / 32
                out[p * 2 + tt, at] = math.cos(angle)
                out[64 + p * 2 + tt, at] = math.sin(angle)
    n = np.arange(64)
    angle = 2.0 * math.pi * (np.outer(n, np.arange(32)) % 64) / 64
    out[128:192, :32] = np.cos(angle)
    out[192:256, :32] = np.sin(angle)
    angle = 2.0 * math.pi * np.outer(n, n) / 4096
    out[256:320] = np.concatenate([np.cos(angle), np.cos(angle)], 1)
    out[320:384] = np.concatenate([-np.sin(angle), np.sin(angle)], 1)
    w = np.concatenate([n[0::2], n[1::2]])
    angle = 2.0 * math.pi * (np.outer(w, n) % 64) / 64
    out[384:448] = np.concatenate([np.cos(angle), -np.sin(angle)], 1)
    return out.astype(np.float32)


def dot_exact(a, b, contract=((1,), (0,))):
    return lax.dot_general(
        a, b, (contract, ((), ())), precision=lax.Precision.HIGHEST, preferred_element_type=F32
    )


def rotated(x):
    return pltpu.roll(x, 64, 1)


def turned(both, sign):
    half = both.shape[0] // 2
    return both[:half] + sign * rotated(both[half:])


def kernel(
    wig_hbm, sky_hbm, beam_hbm, col_hbm, ell_hbm, ooc_hbm, const_hbm,
    left_ref, right_ref,
    wig, sky, beam, col, ell, ooc, const,
    table, coef, acc, from_y, hy, to_z, from_z, ps, got, key, hot_low, grid,
    in_sem, y_send, y_recv, z_send, z_recv, b_send, b_recv,
):
    e = lax.axis_index("ell")
    b = lax.axis_index("blk")
    y, z = e // 4, e % 4
    x, zh, core = b // 8, (b // 2) % 4, b % 2

    def y_peer(d):
        return (lax.rem(y + d, 4) * 4 + z, b)

    def z_peer(d):
        return (y * 4 + lax.rem(z + d, 4), b)

    def b_peer(d):
        return (e, lax.rem(b + d, BLKS))

    loads = [
        pltpu.make_async_copy(src, dst, in_sem.at[i])
        for i, (src, dst) in enumerate(
            [
                (beam_hbm, beam), (ell_hbm, ell), (col_hbm, col), (sky_hbm, sky),
                (const_hbm, const), (ooc_hbm, ooc), (wig_hbm, wig),
            ]
        )
    ]
    for load in loads:
        load.start()
    barrier = pltpu.get_barrier_semaphore()
    peers = [y_peer(d) for d in range(1, 4)] + [z_peer(d) for d in range(1, 4)]
    peers += [b_peer(d) for d in range(1, BLKS)]
    for peer in peers:
        pl.semaphore_signal(barrier, inc=1, device_id=peer, device_id_type=MESH)
    for load in loads[:-1]:
        load.wait()
    gather_all(sky, beam, col, ell, table, coef)
    loads[-1].wait()
    add_all(wig, col, coef, acc)

    pl.semaphore_wait(barrier, len(peers))

    def y_copy(d):
        there = pl.multiple_of(lax.rem(y + d, 4) * 8, 8)
        return pltpu.make_async_remote_copy(
            src_ref=acc.at[:, pl.ds(there, 8), :], dst_ref=from_y.at[d - 1],
            send_sem=y_send.at[d - 1], recv_sem=y_recv.at[d - 1],
            device_id=y_peer(d), device_id_type=MESH,
        )

    y_copies = [y_copy(d) for d in (2, 1, 3)]
    for copy in y_copies:
        copy.start()

    lane = lax.broadcasted_iota(I32, (16, 128), 1)
    order = ooc[...]
    swapped = rotated(order)
    even = jnp.where(lane < 64, order, swapped)
    odd = jnp.where(lane < 64, swapped, order)
    side = jnp.where(lane < 64, 0, 64)
    key[0] = (even & 63) + side
    key[1] = (odd & 63) + side
    key[2] = even >> 6
    key[3] = odd >> 6
    rows = lax.broadcasted_iota(I32, (128, 128), 0)

    def low_step(a, _):
        hot_low[a, :, 0:128] = (rows == key[0, pl.ds(a, 1), :]).astype(F32).astype(BF16)
        hot_low[a, :, 128:256] = (rows == key[1, pl.ds(a, 1), :]).astype(F32).astype(BF16)
        return 0

    lax.fori_loop(0, 16, low_step, 0)
    grid[...] = jnp.zeros((64, 128), F32)
    to_z[:, 32:40, :] = jnp.zeros((4, 8, 128), F32)

    for copy in y_copies:
        copy.wait_recv()
    mine = pl.multiple_of(y * 8, 8)
    total = acc[:, pl.ds(mine, 8), :] + from_y[0] + from_y[1] + from_y[2]
    hy[...] = total.reshape(K * 8, 128)
    for d in range(4):
        for tt in range(2):
            at = 2 * d + tt
            to_z[d, tt * 16 : tt * 16 + 8, :] = hy[pl.ds(at, 8, stride=8), :]
            to_z[d, tt * 16 + 8 : tt * 16 + 16, :] = hy[pl.ds(64 + at, 8, stride=8), :]
            to_z[d, 32 + tt : 33 + tt, :] = hy[128 + at : 129 + at, :]

    def z_copy(d):
        return pltpu.make_async_remote_copy(
            src_ref=to_z.at[lax.rem(z + d, 4)], dst_ref=from_z.at[d - 1],
            send_sem=z_send.at[d - 1], recv_sem=z_recv.at[d - 1],
            device_id=z_peer(d), device_id_type=MESH,
        )

    z_copies = [z_copy(d) for d in (2, 1, 3)]
    for copy in z_copies:
        copy.start()
    for copy in z_copies:
        copy.wait_recv()
    summed = to_z[z] + from_z[0] + from_z[1] + from_z[2]
    lanes = lax.broadcasted_iota(I32, (1, 128), 1)
    sign = jnp.where(lanes < 64, -1.0, 1.0).astype(F32)
    psi = turned(dot_exact(const[0:128, 0:40], summed), sign)
    for p in range(BLKS):
        ps[p] = psi[2 * p : 2 * p + 2]

    def b_copy(d):
        there = lax.rem(b + d, BLKS)
        return pltpu.make_async_remote_copy(
            src_ref=ps.at[there], dst_ref=got.at[b],
            send_sem=b_send.at[d], recv_sem=b_recv.at[b],
            device_id=b_peer(d), device_id_type=MESH,
        )

    b_copies = [b_copy(d) for d in range(1, BLKS)]
    for copy in b_copies:
        copy.start()
    got[b] = ps[b]

    highs = lax.broadcasted_iota(I32, (32, 128), 0)
    steps = sorted(
        ((dx, dz) for dx in range(4) for dz in range(4)),
        key=lambda s: min(s[0], 4 - s[0]) + 4 * min(s[1], 4 - s[1]),
    )
    for dx, dz in steps:
        chip = lax.rem(x + dx, 4) * 4 + lax.rem(zh + dz, 4)
        for c in range(2):
            source = chip * 2 + c
            arrival = pltpu.make_async_remote_copy(
                src_ref=ps.at[0], dst_ref=got.at[source],
                send_sem=b_send.at[0], recv_sem=b_recv.at[source],
                device_id=(e, source), device_id_type=MESH,
            )
            if (dx, dz) == (0, 0):
                @pl.when(core != c)
                def _():
                    arrival.wait_recv()
            else:
                arrival.wait_recv()
        parts = []
        for c in range(2):
            value = got[chip * 2 + c]
            here = highs == key[2 + c, pl.ds(chip, 1), :]
            spread = jnp.concatenate(
                [jnp.where(here, value[tt : tt + 1, :], 0.0) for tt in range(2)], axis=0
            )
            high = spread.astype(BF16)
            parts.append(jnp.concatenate([high, (spread - high.astype(F32)).astype(BF16)], axis=0))
        placed = lax.dot_general(
            jnp.concatenate(parts, axis=1), hot_low[chip], (((1,), (1,)), ((), ())),
            preferred_element_type=F32,
        )
        grid[...] += placed[0:64] + placed[64:128]

    results = []
    for tt in range(2):
        first = turned(dot_exact(const[128:256, 0:32], grid[tt * 32 : tt * 32 + 32, :]), sign)
        results.append(first * const[256:320, :] + rotated(first) * const[320:384, :])
    last = dot_exact(const[384:448, :], jnp.concatenate(results, axis=0), ((1,), (1,)))
    low, upp = last[0:32], last[32:64]
    left = lax.broadcasted_iota(I32, (32, 128), 1) < 64
    left_ref[0] = jnp.where(left, low, 0.0)
    right_ref[0] = jnp.where(left, 0.0, rotated(upp))
    left_ref[1] = jnp.where(left, rotated(low), 0.0)
    right_ref[1] = jnp.where(left, 0.0, upp)
    for copy in y_copies + z_copies + b_copies:
        copy.wait_send()


def on_device(wigner, sky_alm, beam_blm, slot_col, slot_ell, order_of_column):
    q = wigner.shape[2]
    any_space = pl.BlockSpec(memory_space=pltpu.HBM)
    dma = pltpu.SemaphoreType.DMA
    left, right = pl.pallas_call(
        kernel,
        out_shape=[jax.ShapeDtypeStruct((2, 32, 128), F32)] * 2,
        in_specs=[any_space] * 7,
        out_specs=[pl.BlockSpec(memory_space=pltpu.VMEM)] * 2,
        scratch_shapes=[
            pltpu.VMEM((K, T, q), BF16),
            pltpu.VMEM((2, q), F32),
            pltpu.VMEM((K, 2, 2048), F32),
            pltpu.VMEM((q // 128, 128), I32),
            pltpu.VMEM((q // 128, 128), I32),
            pltpu.VMEM((16, 128), I32),
            pltpu.VMEM((448, 128), F32),
            pltpu.VMEM((16, 40, 256), BF16),
            pltpu.VMEM((2, 24, q), F32),
            pltpu.VMEM((K, T, 128), F32),
            pltpu.VMEM((3, K, 8, 128), F32),
            pltpu.VMEM((K * 8, 128), F32),
            pltpu.VMEM((4, 40, 128), F32),
            pltpu.VMEM((3, 40, 128), F32),
            pltpu.VMEM((BLKS, 2, 128), F32),
            pltpu.VMEM((BLKS, 2, 128), F32),
            pltpu.VMEM((4, 16, 128), I32),
            pltpu.VMEM((16, 128, 256), BF16),
            pltpu.VMEM((64, 128), F32),
            dma((7,)),
            dma((3,)), dma((3,)), dma((3,)), dma((3,)), dma((BLKS,)), dma((BLKS,)),
        ],
        compiler_params=pltpu.CompilerParams(
            collective_id=0, has_side_effects=True, vmem_limit_bytes=40 * 1024 * 1024
        ),
    )(
        *(
            pltpu.with_memory_space_constraint(operand, pltpu.HBM)
            for operand in (
                jnp.transpose(wigner, (1, 0, 2)),
                sky_alm,
                jnp.transpose(beam_blm, (1, 0, 2)),
                slot_col.reshape(q // 128, 128),
                slot_ell.reshape(q // 128, 128),
                order_of_column.reshape(16, 128),
                jnp.asarray(constants()),
            )
        )
    )
    return left.reshape(2, 1, 4096) + right.reshape(2, 1, 4096)


def solution(mesh):
    return jax.shard_map(
        on_device,
        mesh=mesh,
        in_specs=(
            P(None, None, ("ell", "blk")),
            P(None, ("ell", "blk")),
            P(),
            P(("ell", "blk")),
            P(("ell", "blk")),
            P(),
        ),
        out_specs=P("ell", "blk", None),
        check_vma=False,
    )
```

```python
import math

import jax
import jax.numpy as jnp
import numpy as np
from jax import lax
from jax.experimental import pallas as pl
from jax.experimental.pallas import tpu as pltpu
from jax.sharding import PartitionSpec as P

F32, BF16, I32 = jnp.float32, jnp.bfloat16, jnp.int32
MESH = pl.DeviceIdType.MESH
K, T, C = 17, 32, 64
H = 8
BLKS = 32

def build_table(beam, table):
    rows = jnp.concatenate([beam[:, 0, :], beam[:, 1, :], jnp.zeros((6, 2048), F32)], axis=0)
    high = rows.astype(BF16)
    low = (rows - high.astype(F32)).astype(BF16)
    for h in range(16):
        span = slice(h * 128, h * 128 + 128)
        table[h, :, 0:128] = high[:, span]
        table[h, :, 128:256] = low[:, span]


def gather_block(base, table, ell, sky, coef, row, cols):
    n = 128 * cols
    degree = jnp.concatenate([ell[pl.ds(row + c, 1), :] for c in range(cols)], axis=1)
    low = degree & 127
    high = (degree >> 7) - base
    hot = (lax.broadcasted_iota(I32, (128, n), 0) == low).astype(F32).astype(BF16)
    hot = jnp.concatenate([hot, hot], axis=0)
    lhs = table[pl.ds(base, 10)].reshape(10 * 40, 256)
    picked = jnp.dot(lhs, hot, preferred_element_type=F32)
    total = jnp.zeros((40, n), F32)
    for h in range(10):
        total = jnp.where(high == h, picked[h * 40 : h * 40 + 40], total)
    br, bi = total[0:17], total[17:34]
    start = pl.multiple_of(row * 128, 128)
    s0 = sky[0:1, pl.ds(start, n)]
    s1 = sky[1:2, pl.ds(start, n)]
    coef[0, 0:17, pl.ds(start, n)] = s0 * br - s1 * bi
    coef[1, 0:17, pl.ds(start, n)] = s0 * bi + s1 * br


def add_block(wig, coef, col, acc, row, cols):
    lhs = []
    rhs = []
    zero = jnp.zeros((64, 128), BF16)
    for c in range(cols):
        start = pl.multiple_of((row + c) * 128, 128)
        span = pl.ds(start, 128)
        re, im = [], []
        for k in range(K):
            w = wig[k, :, span].astype(F32)
            re.append((w * coef[0, pl.ds(k, 1), span]).astype(BF16))
            im.append((w * coef[1, pl.ds(k, 1), span]).astype(BF16))
        lhs += [jnp.concatenate(re, axis=0), jnp.concatenate(im, axis=0)]
        hot = (lax.broadcasted_iota(I32, (64, 128), 0) == col[pl.ds(row + c, 1), :]).astype(F32).astype(BF16)
        rhs += [jnp.concatenate([hot, zero], axis=0), jnp.concatenate([zero, hot], axis=0)]
    left = jnp.concatenate(lhs, axis=1)
    right = jnp.concatenate(rhs, axis=1)
    part = lax.dot_general(left, right, (((1,), (1,)), ((), ())), preferred_element_type=F32)
    acc[...] += part.reshape(K, T, 128)


def gather_all(sky, beam, col, ell, table, coef):
    build_table(beam, table)
    base = jnp.minimum(jnp.min(jnp.where(col[...] >= 0, ell[...], 2047)) >> 7, 6)
    gather_block(base, table, ell, sky, coef, 0, ell.shape[0])


def add_all(wig, col, coef, acc):
    acc[...] = jnp.zeros((K, T, 128), F32)
    add_block(wig, coef, col, acc, 0, col.shape[0])


def constants():
    out = np.zeros((448, 128), np.float64)
    for p in range(32):
        for tt in range(2):
            for k in range(K):
                at = tt * H + k if k < H else 2 * k + tt
                angle = 2.0 * math.pi * (k * p % 32) / 32
                out[p * 2 + tt, at] = math.cos(angle)
                out[64 + p * 2 + tt, at] = math.sin(angle)
    n = np.arange(64)
    angle = 2.0 * math.pi * (np.outer(n, np.arange(32)) % 64) / 64
    out[128:192, :32] = np.cos(angle)
    out[192:256, :32] = np.sin(angle)
    angle = 2.0 * math.pi * np.outer(n, n) / 4096
    out[256:320] = np.concatenate([np.cos(angle), np.cos(angle)], 1)
    out[320:384] = np.concatenate([-np.sin(angle), np.sin(angle)], 1)
    w = np.concatenate([n[0::2], n[1::2]])
    angle = 2.0 * math.pi * (np.outer(w, n) % 64) / 64
    out[384:448] = np.concatenate([np.cos(angle), -np.sin(angle)], 1)
    return out.astype(np.float32)


def dot_exact(a, b, contract=((1,), (0,))):
    return lax.dot_general(
        a, b, (contract, ((), ())), precision=lax.Precision.HIGHEST, preferred_element_type=F32
    )


def rotated(x):
    return pltpu.roll(x, 64, 1)


def turned(both, sign):
    half = both.shape[0] // 2
    return both[:half] + sign * rotated(both[half:])


def kernel(
    wig_hbm, sky_hbm, beam_hbm, col_hbm, ell_hbm, ooc_hbm, const_hbm,
    left_ref, right_ref,
    wig, sky, beam, col, ell, ooc, const,
    table, coef, acc, to_ell, from_ell, from_y, by_cycle, to_z, from_z, summed, ps, got, key, hot_low, grid,
    in_sem, e_send, e_recv, y_send, y_recv, z_send, z_recv, b_send, b_recv,
):
    e = lax.axis_index("ell")
    b = lax.axis_index("blk")
    y, z = e // 4, e % 4
    x, zh, core = b // 8, (b // 2) % 4, b % 2

    def others(order, place):
        return [
            jnp.where(place <= i, order[i + 1], order[i]).astype(I32) for i in range(len(order) - 1)
        ]

    def swap(i):
        return i + (i // 2) * (5 - 2 * i)

    owners = others([there * 4 + at for at in range(4) for there in range(4)], z * 4 + y)
    chips = [xs * 4 + zs for zs in (0, 1, 3, 2) for xs in (0, 1, 3, 2)]
    members = others(
        [chip * 2 + c for chip in chips for c in (1, 0)], swap(zh) * 8 + swap(x) * 2 + 1 - core
    )
    rows_y = others(list(range(4)), y)
    runs_z = others(list(range(4)), z)

    loads = [
        pltpu.make_async_copy(src, dst, in_sem.at[i])
        for i, (src, dst) in enumerate(
            [
                (beam_hbm, beam), (ell_hbm, ell), (col_hbm, col), (sky_hbm, sky),
                (const_hbm, const), (ooc_hbm, ooc), (wig_hbm, wig),
            ]
        )
    ]
    for load in loads:
        load.start()
    barrier = pltpu.get_barrier_semaphore()
    peers = [(owner, b) for owner in owners]
    peers += [(e, there) for there in members]
    for peer in reversed(peers):
        pl.semaphore_signal(barrier, inc=1, device_id=peer, device_id_type=MESH)
    for load in loads[:-1]:
        load.wait()
    gather_all(sky, beam, col, ell, table, coef)
    loads[-1].wait()
    add_all(wig, col, coef, acc)

    pl.semaphore_wait(barrier, len(peers))

    def y_copy(i):
        there = rows_y[i]
        return pltpu.make_async_remote_copy(
            src_ref=acc.at[0:H, pl.ds(pl.multiple_of(there * 8, 8), 8), :], dst_ref=from_y.at[y],
            send_sem=y_send.at[i], recv_sem=y_recv.at[y],
            device_id=(there * 4 + z, b), device_id_type=MESH,
        )

    y_copies = [y_copy(i) for i in range(3)]
    for copy in y_copies:
        copy.start()
    for k in range(H, K):
        for owner in range(16):
            to_ell[owner, k - H] = acc[k, 2 * owner : 2 * owner + 2, :]

    def e_copy(i):
        return pltpu.make_async_remote_copy(
            src_ref=to_ell.at[owners[i]], dst_ref=from_ell.at[e],
            send_sem=e_send.at[i], recv_sem=e_recv.at[e],
            device_id=(owners[i], b), device_id_type=MESH,
        )

    e_copies = [e_copy(i) for i in range(15)]
    for copy in e_copies:
        copy.start()

    lane = lax.broadcasted_iota(I32, (16, 128), 1)
    order = ooc[...]
    swapped = rotated(order)
    even = jnp.where(lane < 64, order, swapped)
    odd = jnp.where(lane < 64, swapped, order)
    side = jnp.where(lane < 64, 0, 64)
    key[0] = (even & 63) + side
    key[1] = (odd & 63) + side
    key[2] = even >> 6
    key[3] = odd >> 6
    rows = lax.broadcasted_iota(I32, (128, 128), 0)

    def low_step(a, _):
        hot_low[a, :, 0:128] = (rows == key[0, pl.ds(a, 1), :]).astype(F32).astype(BF16)
        hot_low[a, :, 128:256] = (rows == key[1, pl.ds(a, 1), :]).astype(F32).astype(BF16)
        return 0

    lax.fori_loop(0, 16, low_step, 0)
    grid[...] = jnp.zeros((64, 128), F32)
    summed[32:40, :] = jnp.zeros((8, 128), F32)

    mine = acc[0:H, pl.ds(pl.multiple_of(y * 8, 8), 8), :]
    for there in rows_y:
        pltpu.make_async_remote_copy(
            src_ref=from_y.at[0], dst_ref=from_y.at[there],
            send_sem=y_send.at[0], recv_sem=y_recv.at[there],
            device_id=(there * 4 + z, b), device_id_type=MESH,
        ).wait_recv()
        mine = mine + from_y[there]
    by_cycle[...] = mine.reshape(H * 8, 128)
    for d in range(4):
        for tt in range(2):
            to_z[d, tt * 8 : tt * 8 + 8, :] = by_cycle[pl.ds(2 * d + tt, 8, stride=8), :]

    def z_copy(i):
        there = runs_z[i]
        return pltpu.make_async_remote_copy(
            src_ref=to_z.at[there], dst_ref=from_z.at[z],
            send_sem=z_send.at[i], recv_sem=z_recv.at[z],
            device_id=(y * 4 + there, b), device_id_type=MESH,
        )

    z_copies = [z_copy(i) for i in range(3)]
    for copy in z_copies:
        copy.start()
    total = to_ell[e]
    for owner in reversed(owners):
        pltpu.make_async_remote_copy(
            src_ref=to_ell.at[0], dst_ref=from_ell.at[owner],
            send_sem=e_send.at[0], recv_sem=e_recv.at[owner],
            device_id=(owner, b), device_id_type=MESH,
        ).wait_recv()
        total = total + from_ell[owner]
    for k in range(H, K):
        summed[2 * k : 2 * k + 2, :] = total[k - H]
    joined = to_z[z]
    for there in runs_z:
        pltpu.make_async_remote_copy(
            src_ref=to_z.at[0], dst_ref=from_z.at[there],
            send_sem=z_send.at[0], recv_sem=z_recv.at[there],
            device_id=(y * 4 + there, b), device_id_type=MESH,
        ).wait_recv()
        joined = joined + from_z[there]
    summed[0 : 2 * H, :] = joined
    lanes = lax.broadcasted_iota(I32, (1, 128), 1)
    sign = jnp.where(lanes < 64, -1.0, 1.0).astype(F32)
    psi = turned(dot_exact(const[0:128, 0:40], summed[...]), sign)
    for p in range(BLKS):
        ps[p] = psi[2 * p : 2 * p + 2]

    def b_copy(i):
        there = members[i]
        return pltpu.make_async_remote_copy(
            src_ref=ps.at[there], dst_ref=got.at[b],
            send_sem=b_send.at[i], recv_sem=b_recv.at[b],
            device_id=(e, there), device_id_type=MESH,
        )

    b_copies = [b_copy(i) for i in range(BLKS - 1)]
    for copy in b_copies:
        copy.start()
    got[b] = ps[b]

    highs = lax.broadcasted_iota(I32, (32, 128), 0)
    for chip in chips:
        for c in range(2):
            source = chip * 2 + c
            arrival = pltpu.make_async_remote_copy(
                src_ref=ps.at[0], dst_ref=got.at[source],
                send_sem=b_send.at[0], recv_sem=b_recv.at[source],
                device_id=(e, members[0]), device_id_type=MESH,
            )

            @pl.when(b != source)
            def _():
                arrival.wait_recv()

        parts = []
        for c in range(2):
            value = got[chip * 2 + c]
            here = highs == key[2 + c, chip : chip + 1, :]
            spread = jnp.concatenate(
                [jnp.where(here, value[tt : tt + 1, :], 0.0) for tt in range(2)], axis=0
            )
            high = spread.astype(BF16)
            parts.append(jnp.concatenate([high, (spread - high.astype(F32)).astype(BF16)], axis=0))
        placed = lax.dot_general(
            jnp.concatenate(parts, axis=1), hot_low[chip], (((1,), (1,)), ((), ())),
            preferred_element_type=F32,
        )
        grid[...] += placed[0:64] + placed[64:128]

    results = []
    for tt in range(2):
        first = turned(dot_exact(const[128:256, 0:32], grid[tt * 32 : tt * 32 + 32, :]), sign)
        results.append(first * const[256:320, :] + rotated(first) * const[320:384, :])
    last = dot_exact(const[384:448, :], jnp.concatenate(results, axis=0), ((1,), (1,)))
    low, upp = last[0:32], last[32:64]
    left = lax.broadcasted_iota(I32, (32, 128), 1) < 64
    left_ref[0] = jnp.where(left, low, 0.0)
    right_ref[0] = jnp.where(left, 0.0, rotated(upp))
    left_ref[1] = jnp.where(left, rotated(low), 0.0)
    right_ref[1] = jnp.where(left, 0.0, upp)
    for copy in y_copies + z_copies + e_copies + b_copies:
        copy.wait_send()


def on_device(wigner, sky_alm, beam_blm, slot_col, slot_ell, order_of_column):
    q = wigner.shape[2]
    any_space = pl.BlockSpec(memory_space=pltpu.HBM)
    dma = pltpu.SemaphoreType.DMA
    left, right = pl.pallas_call(
        kernel,
        out_shape=[jax.ShapeDtypeStruct((2, 32, 128), F32)] * 2,
        in_specs=[any_space] * 7,
        out_specs=[pl.BlockSpec(memory_space=pltpu.VMEM)] * 2,
        scratch_shapes=[
            pltpu.VMEM((K, T, q), BF16),
            pltpu.VMEM((2, q), F32),
            pltpu.VMEM((K, 2, 2048), F32),
            pltpu.VMEM((q // 128, 128), I32),
            pltpu.VMEM((q // 128, 128), I32),
            pltpu.VMEM((16, 128), I32),
            pltpu.VMEM((448, 128), F32),
            pltpu.VMEM((16, 40, 256), BF16),
            pltpu.VMEM((2, 24, q), F32),
            pltpu.VMEM((K, T, 128), F32),
            pltpu.VMEM((16, K - H, 2, 128), F32),
            pltpu.VMEM((16, K - H, 2, 128), F32),
            pltpu.VMEM((4, H, 8, 128), F32),
            pltpu.VMEM((H * 8, 128), F32),
            pltpu.VMEM((4, 2 * H, 128), F32),
            pltpu.VMEM((4, 2 * H, 128), F32),
            pltpu.VMEM((40, 128), F32),
            pltpu.VMEM((BLKS, 2, 128), F32),
            pltpu.VMEM((BLKS, 2, 128), F32),
            pltpu.VMEM((4, 16, 128), I32),
            pltpu.VMEM((16, 128, 256), BF16),
            pltpu.VMEM((64, 128), F32),
            dma((7,)),
            dma((15,)), dma((16,)), dma((3,)), dma((4,)), dma((3,)), dma((4,)), dma((BLKS,)), dma((BLKS,)),
        ],
        compiler_params=pltpu.CompilerParams(
            collective_id=0, has_side_effects=True, vmem_limit_bytes=40 * 1024 * 1024
        ),
    )(
        *(
            pltpu.with_memory_space_constraint(operand, pltpu.HBM)
            for operand in (
                jnp.transpose(wigner, (1, 0, 2)),
                sky_alm,
                jnp.transpose(beam_blm, (1, 0, 2)),
                slot_col.reshape(q // 128, 128),
                slot_ell.reshape(q // 128, 128),
                order_of_column.reshape(16, 128),
                jnp.asarray(constants()),
            )
        )
    )
    return left.reshape(2, 1, 4096) + right.reshape(2, 1, 4096)


def solution(mesh):
    return jax.shard_map(
        on_device,
        mesh=mesh,
        in_specs=(
            P(None, None, ("ell", "blk")),
            P(None, ("ell", "blk")),
            P(),
            P(("ell", "blk")),
            P(("ell", "blk")),
            P(),
        ),
        out_specs=P("ell", "blk", None),
        check_vma=False,
    )
```

```python
import math

import jax
import jax.numpy as jnp
import numpy as np
from jax import lax
from jax.experimental import pallas as pl
from jax.experimental.pallas import tpu as pltpu
from jax.sharding import PartitionSpec as P

F32, BF16, I32 = jnp.float32, jnp.bfloat16, jnp.int32
MESH = pl.DeviceIdType.MESH
K, T, C = 17, 32, 64
H = 8
BLKS = 32

def build_table(beam, table):
    rows = jnp.concatenate([beam[:, 0, :], beam[:, 1, :], jnp.zeros((6, 2048), F32)], axis=0)
    high = rows.astype(BF16)
    low = (rows - high.astype(F32)).astype(BF16)
    for h in range(16):
        span = slice(h * 128, h * 128 + 128)
        table[h, :, 0:128] = high[:, span]
        table[h, :, 128:256] = low[:, span]


def gather_block(base, table, ell, sky, coef, row, cols):
    n = 128 * cols
    degree = jnp.concatenate([ell[pl.ds(row + c, 1), :] for c in range(cols)], axis=1)
    low = degree & 127
    high = (degree >> 7) - base
    hot = (lax.broadcasted_iota(I32, (128, n), 0) == low).astype(F32).astype(BF16)
    hot = jnp.concatenate([hot, hot], axis=0)
    lhs = table[pl.ds(base, 10)].reshape(10 * 40, 256)
    picked = jnp.dot(lhs, hot, preferred_element_type=F32)
    total = jnp.zeros((40, n), F32)
    for h in range(10):
        total = jnp.where(high == h, picked[h * 40 : h * 40 + 40], total)
    br, bi = total[0:17], total[17:34]
    start = pl.multiple_of(row * 128, 128)
    s0 = sky[0:1, pl.ds(start, n)]
    s1 = sky[1:2, pl.ds(start, n)]
    coef[0, 0:17, pl.ds(start, n)] = s0 * br - s1 * bi
    coef[1, 0:17, pl.ds(start, n)] = s0 * bi + s1 * br


def add_block(wig, coef, col, acc, row, cols):
    lhs = []
    rhs = []
    zero = jnp.zeros((64, 128), BF16)
    for c in range(cols):
        start = pl.multiple_of((row + c) * 128, 128)
        span = pl.ds(start, 128)
        re, im = [], []
        for k in range(K):
            w = wig[k, :, span].astype(F32)
            re.append((w * coef[0, pl.ds(k, 1), span]).astype(BF16))
            im.append((w * coef[1, pl.ds(k, 1), span]).astype(BF16))
        lhs += [jnp.concatenate(re, axis=0), jnp.concatenate(im, axis=0)]
        hot = (lax.broadcasted_iota(I32, (64, 128), 0) == col[pl.ds(row + c, 1), :]).astype(F32).astype(BF16)
        rhs += [jnp.concatenate([hot, zero], axis=0), jnp.concatenate([zero, hot], axis=0)]
    left = jnp.concatenate(lhs, axis=1)
    right = jnp.concatenate(rhs, axis=1)
    part = lax.dot_general(left, right, (((1,), (1,)), ((), ())), preferred_element_type=F32)
    acc[...] += part.reshape(K, T, 128)


def gather_all(sky, beam, col, ell, table, coef):
    build_table(beam, table)
    base = jnp.minimum(jnp.min(jnp.where(col[...] >= 0, ell[...], 2047)) >> 7, 6)
    gather_block(base, table, ell, sky, coef, 0, ell.shape[0])


def add_all(wig, col, coef, acc):
    acc[...] = jnp.zeros((K, T, 128), F32)
    add_block(wig, coef, col, acc, 0, col.shape[0])


def constants():
    out = np.zeros((448, 128), np.float64)
    for p in range(32):
        for tt in range(2):
            for k in range(K):
                at = tt * H + k if k < H else 2 * k + tt
                angle = 2.0 * math.pi * (k * p % 32) / 32
                out[p * 2 + tt, at] = math.cos(angle)
                out[64 + p * 2 + tt, at] = math.sin(angle)
    n = np.arange(64)
    angle = 2.0 * math.pi * (np.outer(n, np.arange(32)) % 64) / 64
    out[128:192, :32] = np.cos(angle)
    out[192:256, :32] = np.sin(angle)
    angle = 2.0 * math.pi * np.outer(n, n) / 4096
    out[256:320] = np.concatenate([np.cos(angle), np.cos(angle)], 1)
    out[320:384] = np.concatenate([-np.sin(angle), np.sin(angle)], 1)
    w = np.concatenate([n[0::2], n[1::2]])
    angle = 2.0 * math.pi * (np.outer(w, n) % 64) / 64
    out[384:448] = np.concatenate([np.cos(angle), -np.sin(angle)], 1)
    return out.astype(np.float32)


def dot_exact(a, b, contract=((1,), (0,))):
    return lax.dot_general(
        a, b, (contract, ((), ())), precision=lax.Precision.HIGHEST, preferred_element_type=F32
    )


def rotated(x):
    return pltpu.roll(x, 64, 1)


def turned(both, sign):
    half = both.shape[0] // 2
    return both[:half] + sign * rotated(both[half:])


def kernel(
    wig_hbm, sky_hbm, beam_hbm, col_hbm, ell_hbm, ooc_hbm, const_hbm,
    left_ref, right_ref,
    wig, sky, beam, col, ell, ooc, const,
    table, coef, acc, to_ell, from_ell, from_y, by_cycle, to_z, from_z, summed, ps, got, key, hot_low, grid,
    in_sem, e_send, e_recv, y_send, y_recv, z_send, z_recv, b_send, b_recv,
):
    e = lax.axis_index("ell")
    b = lax.axis_index("blk")
    y, z = e // 4, e % 4
    x, zh, core = b // 8, (b // 2) % 4, b % 2

    turned_run = zh == 2
    other = y * 4 + 3 - z

    def others(order, place):
        return [
            jnp.where(place <= i, order[i + 1], order[i]).astype(I32) for i in range(len(order) - 1)
        ]

    def swap(i):
        return i + (i // 2) * (5 - 2 * i)

    def both(order, turned_order, place):
        return [
            jnp.where(turned_run, there, here).astype(I32)
            for here, there in zip(others(order, place), others(turned_order, place))
        ]

    place_z = jnp.where(turned_run, 3 - z, z).astype(I32)
    cycles = y * 4 + place_z
    owned = others([there * 4 + at for at in range(4) for there in range(4)], place_z * 4 + y)
    owners = both(
        [there * 4 + at for at in range(4) for there in range(4)],
        [there * 4 + 3 - at for at in range(4) for there in range(4)],
        place_z * 4 + y,
    )
    chips = [xs * 4 + zs for zs in (0, 1, 3, 2) for xs in (0, 1, 3, 2)]
    place_b = swap(zh) * 8 + swap(x) * 2 + 1 - core
    members = others([chip * 2 + c for chip in chips for c in (1, 0)], place_b)
    member_turned = others([int(chip % 4 == 2) for chip in chips for c in (1, 0)], place_b)
    rows_y = others(list(range(4)), y)
    cycles_z = others(list(range(4)), place_z)
    runs_z = both(list(range(4)), [3 - at for at in range(4)], place_z)

    loads = [
        pltpu.make_async_copy(src, dst, in_sem.at[i])
        for i, (src, dst) in enumerate(
            [
                (beam_hbm, beam), (ell_hbm, ell), (col_hbm, col), (sky_hbm, sky),
                (const_hbm, const), (ooc_hbm, ooc), (wig_hbm, wig),
            ]
        )
    ]
    for load in loads:
        load.start()
    barrier = pltpu.get_barrier_semaphore()
    peers = [(owner, b) for owner in owners]
    peers += [
        (jnp.where(flag == 1, other, e).astype(I32), there)
        for there, flag in zip(members, member_turned)
    ]
    for peer in reversed(peers):
        pl.semaphore_signal(barrier, inc=1, device_id=peer, device_id_type=MESH)

    @pl.when(turned_run)
    def _():
        pl.semaphore_signal(barrier, inc=1, device_id=(other, b), device_id_type=MESH)
    for load in loads[:-1]:
        load.wait()
    gather_all(sky, beam, col, ell, table, coef)
    loads[-1].wait()
    add_all(wig, col, coef, acc)

    pl.semaphore_wait(barrier, len(peers) + jnp.where(turned_run, 1, 0).astype(I32))

    def y_copy(i):
        there = rows_y[i]
        return pltpu.make_async_remote_copy(
            src_ref=acc.at[0:H, pl.ds(pl.multiple_of(there * 8, 8), 8), :], dst_ref=from_y.at[y],
            send_sem=y_send.at[i], recv_sem=y_recv.at[y],
            device_id=(there * 4 + z, b), device_id_type=MESH,
        )

    y_copies = [y_copy(i) for i in range(3)]
    for copy in y_copies:
        copy.start()
    for k in range(H, K):
        for owner in range(16):
            to_ell[owner, k - H] = acc[k, 2 * owner : 2 * owner + 2, :]

    def e_copy(i):
        return pltpu.make_async_remote_copy(
            src_ref=to_ell.at[owned[i]], dst_ref=from_ell.at[e],
            send_sem=e_send.at[0], recv_sem=e_recv.at[e],
            device_id=(owners[i], b), device_id_type=MESH,
        )

    e_copies = [e_copy(i) for i in range(15)]
    for copy in e_copies:
        copy.start()

    lane = lax.broadcasted_iota(I32, (16, 128), 1)
    order = ooc[...]
    swapped = rotated(order)
    even = jnp.where(lane < 64, order, swapped)
    odd = jnp.where(lane < 64, swapped, order)
    side = jnp.where(lane < 64, 0, 64)
    key[0] = (even & 63) + side
    key[1] = (odd & 63) + side
    key[2] = even >> 6
    key[3] = odd >> 6
    rows = lax.broadcasted_iota(I32, (128, 128), 0)

    def low_step(a, _):
        hot_low[a, :, 0:128] = (rows == key[0, pl.ds(a, 1), :]).astype(F32).astype(BF16)
        hot_low[a, :, 128:256] = (rows == key[1, pl.ds(a, 1), :]).astype(F32).astype(BF16)
        return 0

    lax.fori_loop(0, 16, low_step, 0)
    grid[...] = jnp.zeros((64, 128), F32)
    summed[32:40, :] = jnp.zeros((8, 128), F32)

    mine = acc[0:H, pl.ds(pl.multiple_of(y * 8, 8), 8), :]
    for there in rows_y:
        pltpu.make_async_remote_copy(
            src_ref=from_y.at[0], dst_ref=from_y.at[there],
            send_sem=y_send.at[0], recv_sem=y_recv.at[there],
            device_id=(there * 4 + z, b), device_id_type=MESH,
        ).wait_recv()
        mine = mine + from_y[there]
    by_cycle[...] = mine.reshape(H * 8, 128)
    for d in range(4):
        for tt in range(2):
            to_z[d, tt * 8 : tt * 8 + 8, :] = by_cycle[pl.ds(2 * d + tt, 8, stride=8), :]

    def z_copy(i):
        there = runs_z[i]
        return pltpu.make_async_remote_copy(
            src_ref=to_z.at[cycles_z[i]], dst_ref=from_z.at[z],
            send_sem=z_send.at[i], recv_sem=z_recv.at[z],
            device_id=(y * 4 + there, b), device_id_type=MESH,
        )

    z_copies = [z_copy(i) for i in range(3)]
    for copy in z_copies:
        copy.start()
    total = to_ell[cycles]
    for owner in reversed(owners):
        pltpu.make_async_remote_copy(
            src_ref=to_ell.at[0], dst_ref=from_ell.at[owner],
            send_sem=e_send.at[0], recv_sem=e_recv.at[owner],
            device_id=(owner, b), device_id_type=MESH,
        ).wait_recv()
        total = total + from_ell[owner]
    for k in range(H, K):
        summed[2 * k : 2 * k + 2, :] = total[k - H]
    joined = to_z[place_z]
    for there in runs_z:
        pltpu.make_async_remote_copy(
            src_ref=to_z.at[0], dst_ref=from_z.at[there],
            send_sem=z_send.at[0], recv_sem=z_recv.at[there],
            device_id=(y * 4 + there, b), device_id_type=MESH,
        ).wait_recv()
        joined = joined + from_z[there]
    summed[0 : 2 * H, :] = joined
    lanes = lax.broadcasted_iota(I32, (1, 128), 1)
    sign = jnp.where(lanes < 64, -1.0, 1.0).astype(F32)
    psi = turned(dot_exact(const[0:128, 0:40], summed[...]), sign)
    for p in range(BLKS):
        ps[p] = psi[2 * p : 2 * p + 2]

    def b_copy(i):
        there = members[i]
        return pltpu.make_async_remote_copy(
            src_ref=ps.at[there], dst_ref=got.at[b],
            send_sem=b_send.at[0], recv_sem=b_recv.at[b],
            device_id=(cycles, there), device_id_type=MESH,
        )

    b_copies = [b_copy(i) for i in range(BLKS - 1)]
    for copy in b_copies:
        copy.start()
    home = pltpu.make_async_remote_copy(
        src_ref=ps.at[b], dst_ref=got.at[b],
        send_sem=b_send.at[1], recv_sem=b_recv.at[b],
        device_id=(other, b), device_id_type=MESH,
    )

    @pl.when(turned_run)
    def _():
        home.start()

    @pl.when(zh != 2)
    def _():
        got[b] = ps[b]


    highs = lax.broadcasted_iota(I32, (32, 128), 0)
    for chip in chips:
        for c in range(2):
            source = chip * 2 + c
            arrival = pltpu.make_async_remote_copy(
                src_ref=ps.at[0], dst_ref=got.at[source],
                send_sem=b_send.at[0], recv_sem=b_recv.at[source],
                device_id=(e, members[0]), device_id_type=MESH,
            )

            @pl.when((b != source) | turned_run)
            def _():
                arrival.wait_recv()

        parts = []
        for c in range(2):
            value = got[chip * 2 + c]
            here = highs == key[2 + c, chip : chip + 1, :]
            spread = jnp.concatenate(
                [jnp.where(here, value[tt : tt + 1, :], 0.0) for tt in range(2)], axis=0
            )
            high = spread.astype(BF16)
            parts.append(jnp.concatenate([high, (spread - high.astype(F32)).astype(BF16)], axis=0))
        placed = lax.dot_general(
            jnp.concatenate(parts, axis=1), hot_low[chip], (((1,), (1,)), ((), ())),
            preferred_element_type=F32,
        )
        grid[...] += placed[0:64] + placed[64:128]

    results = []
    for tt in range(2):
        first = turned(dot_exact(const[128:256, 0:32], grid[tt * 32 : tt * 32 + 32, :]), sign)
        results.append(first * const[256:320, :] + rotated(first) * const[320:384, :])
    last = dot_exact(const[384:448, :], jnp.concatenate(results, axis=0), ((1,), (1,)))
    low, upp = last[0:32], last[32:64]
    left = lax.broadcasted_iota(I32, (32, 128), 1) < 64
    left_ref[0] = jnp.where(left, low, 0.0)
    right_ref[0] = jnp.where(left, 0.0, rotated(upp))
    left_ref[1] = jnp.where(left, rotated(low), 0.0)
    right_ref[1] = jnp.where(left, 0.0, upp)
    for copy in y_copies + z_copies:
        copy.wait_send()
    pltpu.make_async_remote_copy(
        src_ref=to_ell.at[0:15], dst_ref=from_ell.at[0:15], send_sem=e_send.at[0],
        recv_sem=e_recv.at[0], device_id=(owners[0], b), device_id_type=MESH,
    ).wait_send()
    pltpu.make_async_remote_copy(
        src_ref=ps.at[0 : BLKS - 1], dst_ref=got.at[0 : BLKS - 1], send_sem=b_send.at[0],
        recv_sem=b_recv.at[0], device_id=(e, members[0]), device_id_type=MESH,
    ).wait_send()

    @pl.when(turned_run)
    def _():
        home.wait_send()


def on_device(wigner, sky_alm, beam_blm, slot_col, slot_ell, order_of_column):
    q = wigner.shape[2]
    any_space = pl.BlockSpec(memory_space=pltpu.HBM)
    dma = pltpu.SemaphoreType.DMA
    left, right = pl.pallas_call(
        kernel,
        out_shape=[jax.ShapeDtypeStruct((2, 32, 128), F32)] * 2,
        in_specs=[any_space] * 7,
        out_specs=[pl.BlockSpec(memory_space=pltpu.VMEM)] * 2,
        scratch_shapes=[
            pltpu.VMEM((K, T, q), BF16),
            pltpu.VMEM((2, q), F32),
            pltpu.VMEM((K, 2, 2048), F32),
            pltpu.VMEM((q // 128, 128), I32),
            pltpu.VMEM((q // 128, 128), I32),
            pltpu.VMEM((16, 128), I32),
            pltpu.VMEM((448, 128), F32),
            pltpu.VMEM((16, 40, 256), BF16),
            pltpu.VMEM((2, 24, q), F32),
            pltpu.VMEM((K, T, 128), F32),
            pltpu.VMEM((16, K - H, 2, 128), F32),
            pltpu.VMEM((16, K - H, 2, 128), F32),
            pltpu.VMEM((4, H, 8, 128), F32),
            pltpu.VMEM((H * 8, 128), F32),
            pltpu.VMEM((4, 2 * H, 128), F32),
            pltpu.VMEM((4, 2 * H, 128), F32),
            pltpu.VMEM((40, 128), F32),
            pltpu.VMEM((BLKS, 2, 128), F32),
            pltpu.VMEM((BLKS, 2, 128), F32),
            pltpu.VMEM((4, 16, 128), I32),
            pltpu.VMEM((16, 128, 256), BF16),
            pltpu.VMEM((64, 128), F32),
            dma((7,)),
            dma((1,)), dma((16,)), dma((3,)), dma((4,)), dma((3,)), dma((4,)), dma((2,)), dma((BLKS,)),
        ],
        compiler_params=pltpu.CompilerParams(
            collective_id=0, has_side_effects=True, vmem_limit_bytes=40 * 1024 * 1024
        ),
    )(
        *(
            pltpu.with_memory_space_constraint(operand, pltpu.HBM)
            for operand in (
                jnp.transpose(wigner, (1, 0, 2)),
                sky_alm,
                jnp.transpose(beam_blm, (1, 0, 2)),
                slot_col.reshape(q // 128, 128),
                slot_ell.reshape(q // 128, 128),
                order_of_column.reshape(16, 128),
                jnp.asarray(constants()),
            )
        )
    )
    return left.reshape(2, 1, 4096) + right.reshape(2, 1, 4096)


def solution(mesh):
    return jax.shard_map(
        on_device,
        mesh=mesh,
        in_specs=(
            P(None, None, ("ell", "blk")),
            P(None, ("ell", "blk")),
            P(),
            P(("ell", "blk")),
            P(("ell", "blk")),
            P(),
        ),
        out_specs=P("ell", "blk", None),
        check_vma=False,
    )
```

```python
import math

import jax
import jax.numpy as jnp
import numpy as np
from jax import lax
from jax.experimental import pallas as pl
from jax.experimental.pallas import tpu as pltpu
from jax.sharding import PartitionSpec as P

F32, BF16, I32 = jnp.float32, jnp.bfloat16, jnp.int32
MESH = pl.DeviceIdType.MESH
K, T, C = 17, 32, 64
H = 8
BLKS = 32

def build_table(beam, table):
    rows = jnp.concatenate([beam[:, 0, :], beam[:, 1, :], jnp.zeros((6, 2048), F32)], axis=0)
    high = rows.astype(BF16)
    low = (rows - high.astype(F32)).astype(BF16)
    for h in range(16):
        span = slice(h * 128, h * 128 + 128)
        table[h, :, 0:128] = high[:, span]
        table[h, :, 128:256] = low[:, span]


def gather_block(base, table, ell, sky, coef, row, cols):
    n = 128 * cols
    degree = jnp.concatenate([ell[pl.ds(row + c, 1), :] for c in range(cols)], axis=1)
    low = degree & 127
    high = (degree >> 7) - base
    hot = (lax.broadcasted_iota(I32, (128, n), 0) == low).astype(F32).astype(BF16)
    hot = jnp.concatenate([hot, hot], axis=0)
    lhs = table[pl.ds(base, 10)].reshape(10 * 40, 256)
    picked = jnp.dot(lhs, hot, preferred_element_type=F32)
    total = jnp.zeros((40, n), F32)
    for h in range(10):
        total = jnp.where(high == h, picked[h * 40 : h * 40 + 40], total)
    br, bi = total[0:17], total[17:34]
    start = pl.multiple_of(row * 128, 128)
    s0 = sky[0:1, pl.ds(start, n)]
    s1 = sky[1:2, pl.ds(start, n)]
    coef[0, 0:17, pl.ds(start, n)] = s0 * br - s1 * bi
    coef[1, 0:17, pl.ds(start, n)] = s0 * bi + s1 * br


def add_block(wig, coef, col, acc, row, cols):
    lhs = []
    rhs = []
    zero = jnp.zeros((64, 128), BF16)
    for c in range(cols):
        start = pl.multiple_of((row + c) * 128, 128)
        span = pl.ds(start, 128)
        re, im = [], []
        for k in range(K):
            w = wig[k, :, span].astype(F32)
            re.append((w * coef[0, pl.ds(k, 1), span]).astype(BF16))
            im.append((w * coef[1, pl.ds(k, 1), span]).astype(BF16))
        lhs += [jnp.concatenate(re, axis=0), jnp.concatenate(im, axis=0)]
        hot = (lax.broadcasted_iota(I32, (64, 128), 0) == col[pl.ds(row + c, 1), :]).astype(F32).astype(BF16)
        rhs += [jnp.concatenate([hot, zero], axis=0), jnp.concatenate([zero, hot], axis=0)]
    left = jnp.concatenate(lhs, axis=1)
    right = jnp.concatenate(rhs, axis=1)
    part = lax.dot_general(left, right, (((1,), (1,)), ((), ())), preferred_element_type=F32)
    acc[...] = part.reshape(K, T, 128)


def gather_all(sky, beam, col, ell, table, coef):
    build_table(beam, table)
    base = jnp.minimum(jnp.min(jnp.where(col[...] >= 0, ell[...], 2047)) >> 7, 6)
    gather_block(base, table, ell, sky, coef, 0, ell.shape[0])


def add_all(wig, col, coef, acc):
    add_block(wig, coef, col, acc, 0, col.shape[0])


def constants():
    out = np.zeros((448, 128), np.float64)
    for p in range(32):
        for tt in range(2):
            for k in range(K):
                at = tt * H + k if k < H else 2 * k + tt
                angle = 2.0 * math.pi * (k * p % 32) / 32
                out[p * 2 + tt, at] = math.cos(angle)
                out[64 + p * 2 + tt, at] = math.sin(angle)
    n = np.arange(64)
    angle = 2.0 * math.pi * (np.outer(n, np.arange(32)) % 64) / 64
    out[128:192, :32] = np.cos(angle)
    out[192:256, :32] = np.sin(angle)
    angle = 2.0 * math.pi * np.outer(n, n) / 4096
    out[256:320] = np.concatenate([np.cos(angle), np.cos(angle)], 1)
    out[320:384] = np.concatenate([-np.sin(angle), np.sin(angle)], 1)
    w = np.concatenate([n[0::2], n[1::2]])
    angle = 2.0 * math.pi * (np.outer(w, n) % 64) / 64
    out[384:448] = np.concatenate([np.cos(angle), -np.sin(angle)], 1)
    twist = jnp.asarray(out[256:384].astype(np.float32))
    factors = np.zeros((320, 384), jnp.bfloat16)
    for rows, depth, source in ((128, 48, 0), (128, 32, 128), (64, 128, 384)):
        at = {0: 0, 128: 128, 384: 256}[source]
        exact = out[source : source + rows, :depth]
        high = exact.astype(jnp.bfloat16)
        low = (exact - high.astype(np.float64)).astype(jnp.bfloat16)
        factors[at : at + rows, : 3 * depth] = np.concatenate([high, high, low], axis=1)
    return twist, jnp.asarray(factors)


def two_parts(x):
    high = x.astype(BF16)
    return [high, (x - high.astype(F32)).astype(BF16)]


def three_terms(x, axis):
    high, low = two_parts(x)
    return jnp.concatenate([high, low, high], axis=axis)


def rotated(x):
    return pltpu.roll(x, 64, 1)


def turned(both, sign):
    half = both.shape[0] // 2
    return both[:half] + sign * rotated(both[half:])


def kernel(
    wig_hbm, sky_hbm, beam_hbm, col_hbm, ell_hbm, ooc_hbm, const_hbm, factors_hbm,
    left_ref, right_ref,
    wig, sky, beam, col, ell, ooc, const, factors,
    table, coef, acc, to_ell, from_ell, from_y, by_cycle, to_z, from_z, summed, ps, got, key, hot_low, grid,
    in_sem, e_send, e_recv, y_send, y_recv, z_send, z_recv, b_send, b_recv,
):
    e = lax.axis_index("ell")
    b = lax.axis_index("blk")
    y, z = e // 4, e % 4
    x, zh, core = b // 8, (b // 2) % 4, b % 2

    turned_run = zh == 2
    other = y * 4 + 3 - z

    def others(order, place):
        return [
            jnp.where(place <= i, order[i + 1], order[i]).astype(I32) for i in range(len(order) - 1)
        ]

    def swap(i):
        return i + (i // 2) * (5 - 2 * i)

    def both(order, turned_order, place):
        return [
            jnp.where(turned_run, there, here).astype(I32)
            for here, there in zip(others(order, place), others(turned_order, place))
        ]

    place_z = jnp.where(turned_run, 3 - z, z).astype(I32)
    cycles = y * 4 + place_z
    owned = others([there * 4 + at for at in range(4) for there in range(4)], place_z * 4 + y)
    owners = both(
        [there * 4 + at for at in range(4) for there in range(4)],
        [there * 4 + 3 - at for at in range(4) for there in range(4)],
        place_z * 4 + y,
    )
    chips = [xs * 4 + zs for zs in (0, 1, 3, 2) for xs in (0, 1, 3, 2)]
    place_b = swap(zh) * 8 + swap(x) * 2 + 1 - core
    members = others([chip * 2 + c for chip in chips for c in (1, 0)], place_b)
    member_turned = others([int(chip % 4 == 2) for chip in chips for c in (1, 0)], place_b)
    rows_y = others(list(range(4)), y)
    cycles_z = others(list(range(4)), place_z)
    runs_z = both(list(range(4)), [3 - at for at in range(4)], place_z)

    loads = [
        pltpu.make_async_copy(src, dst, in_sem.at[i])
        for i, (src, dst) in enumerate(
            [
                (beam_hbm, beam), (ell_hbm, ell), (col_hbm, col), (sky_hbm, sky),
                (const_hbm, const), (ooc_hbm, ooc), (factors_hbm, factors), (wig_hbm, wig),
            ]
        )
    ]
    for load in loads:
        load.start()
    barrier = pltpu.get_barrier_semaphore()
    peers = [(owner, b) for owner in owners]
    peers += [
        (jnp.where(flag == 1, other, e).astype(I32), there)
        for there, flag in zip(members, member_turned)
    ]
    for peer in reversed(peers):
        pl.semaphore_signal(barrier, inc=1, device_id=peer, device_id_type=MESH)

    @pl.when(turned_run)
    def _():
        pl.semaphore_signal(barrier, inc=1, device_id=(other, b), device_id_type=MESH)
    for load in loads[:-1]:
        load.wait()
    gather_all(sky, beam, col, ell, table, coef)
    loads[-1].wait()
    add_all(wig, col, coef, acc)

    pl.semaphore_wait(barrier, len(peers) + jnp.where(turned_run, 1, 0).astype(I32))

    def y_copy(i):
        there = rows_y[i]
        return pltpu.make_async_remote_copy(
            src_ref=acc.at[0:H, pl.ds(pl.multiple_of(there * 8, 8), 8), :], dst_ref=from_y.at[y],
            send_sem=y_send.at[i], recv_sem=y_recv.at[y],
            device_id=(there * 4 + z, b), device_id_type=MESH,
        )

    y_copies = [y_copy(i) for i in range(3)]
    for copy in y_copies:
        copy.start()
    for k in range(H, K):
        for owner in range(16):
            to_ell[owner, k - H] = acc[k, 2 * owner : 2 * owner + 2, :]

    def e_copy(i):
        return pltpu.make_async_remote_copy(
            src_ref=to_ell.at[owned[i]], dst_ref=from_ell.at[e],
            send_sem=e_send.at[0], recv_sem=e_recv.at[e],
            device_id=(owners[i], b), device_id_type=MESH,
        )

    e_copies = [e_copy(i) for i in range(15)]
    for copy in e_copies:
        copy.start()

    lane = lax.broadcasted_iota(I32, (16, 128), 1)
    order = ooc[...]
    swapped = rotated(order)
    even = jnp.where(lane < 64, order, swapped)
    odd = jnp.where(lane < 64, swapped, order)
    side = jnp.where(lane < 64, 0, 64)
    key[0] = (even & 63) + side
    key[1] = (odd & 63) + side
    key[2] = even >> 6
    key[3] = odd >> 6
    rows = lax.broadcasted_iota(I32, (128, 128), 0)

    def low_step(a, _):
        hot_low[a, :, 0:128] = (rows == key[0, pl.ds(a, 1), :]).astype(F32).astype(BF16)
        hot_low[a, :, 128:256] = (rows == key[1, pl.ds(a, 1), :]).astype(F32).astype(BF16)
        return 0

    lax.fori_loop(0, 16, low_step, 0)
    grid[...] = jnp.zeros((64, 128), F32)
    summed[32:48, :] = jnp.zeros((16, 128), F32)

    mine = acc[0:H, pl.ds(pl.multiple_of(y * 8, 8), 8), :]
    for there in rows_y:
        pltpu.make_async_remote_copy(
            src_ref=from_y.at[0], dst_ref=from_y.at[there],
            send_sem=y_send.at[0], recv_sem=y_recv.at[there],
            device_id=(there * 4 + z, b), device_id_type=MESH,
        ).wait_recv()
        mine = mine + from_y[there]
    by_cycle[...] = mine.reshape(H * 8, 128)
    for d in range(4):
        for tt in range(2):
            to_z[d, tt * 8 : tt * 8 + 8, :] = by_cycle[pl.ds(2 * d + tt, 8, stride=8), :]

    def z_copy(i):
        there = runs_z[i]
        return pltpu.make_async_remote_copy(
            src_ref=to_z.at[cycles_z[i]], dst_ref=from_z.at[z],
            send_sem=z_send.at[i], recv_sem=z_recv.at[z],
            device_id=(y * 4 + there, b), device_id_type=MESH,
        )

    z_copies = [z_copy(i) for i in range(3)]
    for copy in z_copies:
        copy.start()
    total = to_ell[cycles]
    for owner in reversed(owners):
        pltpu.make_async_remote_copy(
            src_ref=to_ell.at[0], dst_ref=from_ell.at[owner],
            send_sem=e_send.at[0], recv_sem=e_recv.at[owner],
            device_id=(owner, b), device_id_type=MESH,
        ).wait_recv()
        total = total + from_ell[owner]
    for k in range(H, K):
        summed[2 * k : 2 * k + 2, :] = total[k - H]
    joined = to_z[place_z]
    for there in runs_z:
        pltpu.make_async_remote_copy(
            src_ref=to_z.at[0], dst_ref=from_z.at[there],
            send_sem=z_send.at[0], recv_sem=z_recv.at[there],
            device_id=(y * 4 + there, b), device_id_type=MESH,
        ).wait_recv()
        joined = joined + from_z[there]
    summed[0 : 2 * H, :] = joined
    lanes = lax.broadcasted_iota(I32, (1, 128), 1)
    sign = jnp.where(lanes < 64, -1.0, 1.0).astype(F32)
    terms = three_terms(summed[...], 0)
    psi = turned(jnp.dot(factors[0:128, 0:144], terms, preferred_element_type=F32), sign)
    for p in range(BLKS):
        ps[p] = psi[2 * p : 2 * p + 2]

    def b_copy(i):
        there = members[i]
        return pltpu.make_async_remote_copy(
            src_ref=ps.at[there], dst_ref=got.at[b],
            send_sem=b_send.at[0], recv_sem=b_recv.at[b],
            device_id=(cycles, there), device_id_type=MESH,
        )

    b_copies = [b_copy(i) for i in range(BLKS - 1)]
    for copy in b_copies:
        copy.start()
    home = pltpu.make_async_remote_copy(
        src_ref=ps.at[b], dst_ref=got.at[b],
        send_sem=b_send.at[1], recv_sem=b_recv.at[b],
        device_id=(other, b), device_id_type=MESH,
    )

    @pl.when(turned_run)
    def _():
        home.start()

    @pl.when(zh != 2)
    def _():
        got[b] = ps[b]


    highs = lax.broadcasted_iota(I32, (32, 128), 0)
    for first in range(0, 16, 4):
        group = chips[first : first + 4]
        for source in [chip * 2 + c for chip in group for c in range(2)]:
            arrival = pltpu.make_async_remote_copy(
                src_ref=ps.at[0], dst_ref=got.at[source],
                send_sem=b_send.at[0], recv_sem=b_recv.at[source],
                device_id=(e, members[0]), device_id_type=MESH,
            )

            @pl.when((b != source) | turned_run)
            def _():
                arrival.wait_recv()

        parts = []
        for chip in group:
            for c in range(2):
                value = got[chip * 2 + c]
                here = highs == key[2 + c, chip : chip + 1, :]
                spread = jnp.concatenate(
                    [jnp.where(here, value[tt : tt + 1, :], 0.0) for tt in range(2)], axis=0
                )
                parts.append(jnp.concatenate(two_parts(spread), axis=0))
        placed = lax.dot_general(
            jnp.concatenate(parts, axis=1),
            jnp.concatenate([hot_low[chip] for chip in group], axis=1),
            (((1,), (1,)), ((), ())), preferred_element_type=F32,
        )
        grid[...] += placed[0:64] + placed[64:128]

    results = []
    for tt in range(2):
        terms = three_terms(grid[tt * 32 : tt * 32 + 32, :], 0)
        first = turned(jnp.dot(factors[128:256, 0:96], terms, preferred_element_type=F32), sign)
        results.append(three_terms(first * const[0:64, :] + rotated(first) * const[64:128, :], 1))
    last = lax.dot_general(
        factors[256:320, :], jnp.concatenate(results, axis=0), (((1,), (1,)), ((), ())),
        preferred_element_type=F32,
    )
    low, upp = last[0:32], last[32:64]
    left = lax.broadcasted_iota(I32, (32, 128), 1) < 64
    left_ref[0] = jnp.where(left, low, 0.0)
    right_ref[0] = jnp.where(left, 0.0, rotated(upp))
    left_ref[1] = jnp.where(left, rotated(low), 0.0)
    right_ref[1] = jnp.where(left, 0.0, upp)
    for copy in y_copies + z_copies:
        copy.wait_send()
    pltpu.make_async_remote_copy(
        src_ref=to_ell.at[0:15], dst_ref=from_ell.at[0:15], send_sem=e_send.at[0],
        recv_sem=e_recv.at[0], device_id=(owners[0], b), device_id_type=MESH,
    ).wait_send()
    pltpu.make_async_remote_copy(
        src_ref=ps.at[0 : BLKS - 1], dst_ref=got.at[0 : BLKS - 1], send_sem=b_send.at[0],
        recv_sem=b_recv.at[0], device_id=(e, members[0]), device_id_type=MESH,
    ).wait_send()

    @pl.when(turned_run)
    def _():
        home.wait_send()


def on_device(wigner, sky_alm, beam_blm, slot_col, slot_ell, order_of_column):
    q = wigner.shape[2]
    any_space = pl.BlockSpec(memory_space=pltpu.HBM)
    dma = pltpu.SemaphoreType.DMA
    left, right = pl.pallas_call(
        kernel,
        out_shape=[jax.ShapeDtypeStruct((2, 32, 128), F32)] * 2,
        in_specs=[any_space] * 8,
        out_specs=[pl.BlockSpec(memory_space=pltpu.VMEM)] * 2,
        scratch_shapes=[
            pltpu.VMEM((K, T, q), BF16),
            pltpu.VMEM((2, q), F32),
            pltpu.VMEM((K, 2, 2048), F32),
            pltpu.VMEM((q // 128, 128), I32),
            pltpu.VMEM((q // 128, 128), I32),
            pltpu.VMEM((16, 128), I32),
            pltpu.VMEM((128, 128), F32),
            pltpu.VMEM((320, 384), BF16),
            pltpu.VMEM((16, 40, 256), BF16),
            pltpu.VMEM((2, 24, q), F32),
            pltpu.VMEM((K, T, 128), F32),
            pltpu.VMEM((16, K - H, 2, 128), F32),
            pltpu.VMEM((16, K - H, 2, 128), F32),
            pltpu.VMEM((4, H, 8, 128), F32),
            pltpu.VMEM((H * 8, 128), F32),
            pltpu.VMEM((4, 2 * H, 128), F32),
            pltpu.VMEM((4, 2 * H, 128), F32),
            pltpu.VMEM((48, 128), F32),
            pltpu.VMEM((BLKS, 2, 128), F32),
            pltpu.VMEM((BLKS, 2, 128), F32),
            pltpu.VMEM((4, 16, 128), I32),
            pltpu.VMEM((16, 128, 256), BF16),
            pltpu.VMEM((64, 128), F32),
            dma((8,)),
            dma((1,)), dma((16,)), dma((3,)), dma((4,)), dma((3,)), dma((4,)), dma((2,)), dma((BLKS,)),
        ],
        compiler_params=pltpu.CompilerParams(
            collective_id=0, has_side_effects=True, vmem_limit_bytes=40 * 1024 * 1024
        ),
    )(
        *(
            pltpu.with_memory_space_constraint(operand, pltpu.HBM)
            for operand in (
                jnp.transpose(wigner, (1, 0, 2)),
                sky_alm,
                jnp.transpose(beam_blm, (1, 0, 2)),
                slot_col.reshape(q // 128, 128),
                slot_ell.reshape(q // 128, 128),
                order_of_column.reshape(16, 128),
                *constants(),
            )
        )
    )
    return left.reshape(2, 1, 4096) + right.reshape(2, 1, 4096)


def solution(mesh):
    return jax.shard_map(
        on_device,
        mesh=mesh,
        in_specs=(
            P(None, None, ("ell", "blk")),
            P(None, ("ell", "blk")),
            P(),
            P(("ell", "blk")),
            P(("ell", "blk")),
            P(),
        ),
        out_specs=P("ell", "blk", None),
        check_vma=False,
    )
```

```python
import math

import jax
import jax.numpy as jnp
import numpy as np
from jax import lax
from jax.experimental import pallas as pl
from jax.experimental.pallas import tpu as pltpu
from jax.sharding import PartitionSpec as P

F32, BF16, I32 = jnp.float32, jnp.bfloat16, jnp.int32
MESH = pl.DeviceIdType.MESH
K, T, C = 17, 32, 64
H = 8
BLKS = 32

def build_table(beam, table):
    rows = jnp.concatenate([beam[:, 0, :], beam[:, 1, :], jnp.zeros((6, 2048), F32)], axis=0)
    for h in range(16):
        table[h] = rows[:, h * 128 : h * 128 + 128]


def gather_block(base, table, ell, sky, coef, first, last):
    for c in range(first, last):
        degree = ell[c : c + 1, :]
        low = jnp.broadcast_to(degree & 127, (8, 128))
        high = jnp.broadcast_to((degree >> 7) - base, (8, 128))
        hits = [high == h for h in range(10)]
        groups = []
        for g in range(5):
            total = jnp.zeros((8, 128), F32)
            for h in range(10):
                rows = table[base + h, 8 * g : 8 * g + 8, :]
                got = jnp.take_along_axis(rows, low, axis=1, mode="promise_in_bounds")
                total = jnp.where(hits[h], got, total)
            groups.append(total)
        total = jnp.concatenate(groups, axis=0)
        br, bi = total[0:17], total[17:34]
        span = slice(c * 128, c * 128 + 128)
        s0 = sky[0:1, span]
        s1 = sky[1:2, span]
        coef[0, 0:17, span] = s0 * br - s1 * bi
        coef[1, 0:17, span] = s0 * bi + s1 * br


def add_block(wig, coef, col, acc, row, cols):
    lhs = []
    rhs = []
    zero = jnp.zeros((64, 128), BF16)
    for c in range(cols):
        start = pl.multiple_of((row + c) * 128, 128)
        span = pl.ds(start, 128)
        re, im = [], []
        for k in range(K):
            w = wig[k, :, span].astype(F32)
            re.append((w * coef[0, pl.ds(k, 1), span]).astype(BF16))
            im.append((w * coef[1, pl.ds(k, 1), span]).astype(BF16))
        lhs += [jnp.concatenate(re, axis=0), jnp.concatenate(im, axis=0)]
        hot = (lax.broadcasted_iota(I32, (64, 128), 0) == col[pl.ds(row + c, 1), :]).astype(F32).astype(BF16)
        rhs += [jnp.concatenate([hot, zero], axis=0), jnp.concatenate([zero, hot], axis=0)]
    left = jnp.concatenate(lhs, axis=1)
    right = jnp.concatenate(rhs, axis=1)
    part = lax.dot_general(left, right, (((1,), (1,)), ((), ())), preferred_element_type=F32)
    acc[...] = part.reshape(K, T, 128)


def add_all(wig, col, coef, acc):
    add_block(wig, coef, col, acc, 0, col.shape[0])


def constants():
    out = np.zeros((448, 128), np.float64)
    for p in range(32):
        for tt in range(2):
            for k in range(K):
                at = tt * H + k if k < H else 2 * k + tt
                angle = 2.0 * math.pi * (k * p % 32) / 32
                out[p * 2 + tt, at] = math.cos(angle)
                out[64 + p * 2 + tt, at] = math.sin(angle)
    n = np.arange(64)
    angle = 2.0 * math.pi * (np.outer(n, np.arange(32)) % 64) / 64
    out[128:192, :32] = np.cos(angle)
    out[192:256, :32] = np.sin(angle)
    angle = 2.0 * math.pi * np.outer(n, n) / 4096
    out[256:320] = np.concatenate([np.cos(angle), np.cos(angle)], 1)
    out[320:384] = np.concatenate([-np.sin(angle), np.sin(angle)], 1)
    w = np.concatenate([n[0::2], n[1::2]])
    angle = 2.0 * math.pi * (np.outer(w, n) % 64) / 64
    out[384:448] = np.concatenate([np.cos(angle), -np.sin(angle)], 1)
    twist = jnp.asarray(out[256:384].astype(np.float32))
    factors = np.zeros((320, 384), jnp.bfloat16)
    for rows, depth, source in ((128, 48, 0), (128, 32, 128), (64, 128, 384)):
        at = {0: 0, 128: 128, 384: 256}[source]
        exact = out[source : source + rows, :depth]
        high = exact.astype(jnp.bfloat16)
        low = (exact - high.astype(np.float64)).astype(jnp.bfloat16)
        factors[at : at + rows, : 3 * depth] = np.concatenate([high, high, low], axis=1)
    return twist, jnp.asarray(factors)


def two_parts(x):
    high = x.astype(BF16)
    return [high, (x - high.astype(F32)).astype(BF16)]


def three_terms(x, axis):
    high, low = two_parts(x)
    return jnp.concatenate([high, low, high], axis=axis)


def rotated(x):
    return pltpu.roll(x, 64, 1)


def turned(both, sign):
    half = both.shape[0] // 2
    return both[:half] + sign * rotated(both[half:])


def kernel(
    wig_hbm, sky_hbm, beam_hbm, col_hbm, ell_hbm, ooc_hbm, const_hbm, factors_hbm,
    left_ref, right_ref,
    wig, sky, beam, col, ell, ooc, const, factors,
    table, coef, acc, to_ell, from_ell, from_y, by_cycle, to_z, from_z, summed, ps, got, key, hot_low, grid,
    in_sem, e_send, e_recv, y_send, y_recv, z_send, z_recv, b_send, b_recv,
):
    e = lax.axis_index("ell")
    b = lax.axis_index("blk")
    y, z = e // 4, e % 4
    x, zh, core = b // 8, (b // 2) % 4, b % 2

    turned_run = zh == 2
    other = y * 4 + 3 - z

    def others(order, place):
        return [
            jnp.where(place <= i, order[i + 1], order[i]).astype(I32) for i in range(len(order) - 1)
        ]

    def swap(i):
        return i + (i // 2) * (5 - 2 * i)

    def both(order, turned_order, place):
        return [
            jnp.where(turned_run, there, here).astype(I32)
            for here, there in zip(others(order, place), others(turned_order, place))
        ]

    place_z = jnp.where(turned_run, 3 - z, z).astype(I32)
    cycles = y * 4 + place_z
    owned = others([there * 4 + at for at in range(4) for there in range(4)], place_z * 4 + y)
    owners = both(
        [there * 4 + at for at in range(4) for there in range(4)],
        [there * 4 + 3 - at for at in range(4) for there in range(4)],
        place_z * 4 + y,
    )
    chips = [xs * 4 + zs for zs in (0, 1, 3, 2) for xs in (0, 1, 3, 2)]
    place_b = swap(zh) * 8 + swap(x) * 2 + 1 - core
    members = others([chip * 2 + c for chip in chips for c in (1, 0)], place_b)
    member_turned = others([int(chip % 4 == 2) for chip in chips for c in (1, 0)], place_b)
    rows_y = others(list(range(4)), y)
    cycles_z = others(list(range(4)), place_z)
    runs_z = both(list(range(4)), [3 - at for at in range(4)], place_z)

    loads = [
        pltpu.make_async_copy(src, dst, in_sem.at[i])
        for i, (src, dst) in enumerate(
            [
                (beam_hbm, beam), (ell_hbm, ell), (col_hbm, col), (sky_hbm, sky),
                (wig_hbm, wig), (ooc_hbm, ooc), (const_hbm, const), (factors_hbm, factors),
            ]
        )
    ]
    for load in loads:
        load.start()
    barrier = pltpu.get_barrier_semaphore()
    peers = [(owner, b) for owner in owners]
    peers += [
        (jnp.where(flag == 1, other, e).astype(I32), there)
        for there, flag in zip(members, member_turned)
    ]
    for peer in reversed(peers):
        pl.semaphore_signal(barrier, inc=1, device_id=peer, device_id_type=MESH)

    @pl.when(turned_run)
    def _():
        pl.semaphore_signal(barrier, inc=1, device_id=(other, b), device_id_type=MESH)
    for load in loads[:4]:
        load.wait()
    build_table(beam, table)
    base = jnp.minimum(jnp.min(jnp.where(col[...] >= 0, ell[...], 2047)) >> 7, 6)
    tiles = ell.shape[0]
    ahead = 10
    gather_block(base, table, ell, sky, coef, 0, ahead)
    loads[4].wait()
    gather_block(base, table, ell, sky, coef, ahead, tiles)
    add_all(wig, col, coef, acc)

    pl.semaphore_wait(barrier, len(peers) + jnp.where(turned_run, 1, 0).astype(I32))

    def y_copy(i):
        there = rows_y[i]
        return pltpu.make_async_remote_copy(
            src_ref=acc.at[0:H, pl.ds(pl.multiple_of(there * 8, 8), 8), :], dst_ref=from_y.at[y],
            send_sem=y_send.at[i], recv_sem=y_recv.at[y],
            device_id=(there * 4 + z, b), device_id_type=MESH,
        )

    y_copies = [y_copy(i) for i in range(3)]
    for copy in y_copies:
        copy.start()
    for k in range(H, K):
        for owner in range(16):
            to_ell[owner, k - H] = acc[k, 2 * owner : 2 * owner + 2, :]

    def e_copy(i):
        return pltpu.make_async_remote_copy(
            src_ref=to_ell.at[owned[i]], dst_ref=from_ell.at[e],
            send_sem=e_send.at[0], recv_sem=e_recv.at[e],
            device_id=(owners[i], b), device_id_type=MESH,
        )

    e_copies = [e_copy(i) for i in range(15)]
    for copy in e_copies:
        copy.start()

    for load in loads[5:]:
        load.wait()
    lane = lax.broadcasted_iota(I32, (16, 128), 1)
    order = ooc[...]
    swapped = rotated(order)
    even = jnp.where(lane < 64, order, swapped)
    odd = jnp.where(lane < 64, swapped, order)
    side = jnp.where(lane < 64, 0, 64)
    key[0] = (even & 63) + side
    key[1] = (odd & 63) + side
    key[2] = even >> 6
    key[3] = odd >> 6
    rows = lax.broadcasted_iota(I32, (128, 128), 0)

    def low_step(a, _):
        hot_low[a, :, 0:128] = (rows == key[0, pl.ds(a, 1), :]).astype(F32).astype(BF16)
        hot_low[a, :, 128:256] = (rows == key[1, pl.ds(a, 1), :]).astype(F32).astype(BF16)
        return 0

    lax.fori_loop(0, 16, low_step, 0)
    grid[...] = jnp.zeros((64, 128), F32)
    summed[32:48, :] = jnp.zeros((16, 128), F32)

    mine = acc[0:H, pl.ds(pl.multiple_of(y * 8, 8), 8), :]
    for there in rows_y:
        pltpu.make_async_remote_copy(
            src_ref=from_y.at[0], dst_ref=from_y.at[there],
            send_sem=y_send.at[0], recv_sem=y_recv.at[there],
            device_id=(there * 4 + z, b), device_id_type=MESH,
        ).wait_recv()
        mine = mine + from_y[there]
    by_cycle[...] = mine.reshape(H * 8, 128)
    for d in range(4):
        for tt in range(2):
            to_z[d, tt * 8 : tt * 8 + 8, :] = by_cycle[pl.ds(2 * d + tt, 8, stride=8), :]

    def z_copy(i):
        there = runs_z[i]
        return pltpu.make_async_remote_copy(
            src_ref=to_z.at[cycles_z[i]], dst_ref=from_z.at[z],
            send_sem=z_send.at[i], recv_sem=z_recv.at[z],
            device_id=(y * 4 + there, b), device_id_type=MESH,
        )

    z_copies = [z_copy(i) for i in range(3)]
    for copy in z_copies:
        copy.start()
    total = to_ell[cycles]
    for owner in reversed(owners):
        pltpu.make_async_remote_copy(
            src_ref=to_ell.at[0], dst_ref=from_ell.at[owner],
            send_sem=e_send.at[0], recv_sem=e_recv.at[owner],
            device_id=(owner, b), device_id_type=MESH,
        ).wait_recv()
        total = total + from_ell[owner]
    for k in range(H, K):
        summed[2 * k : 2 * k + 2, :] = total[k - H]
    joined = to_z[place_z]
    for there in runs_z:
        pltpu.make_async_remote_copy(
            src_ref=to_z.at[0], dst_ref=from_z.at[there],
            send_sem=z_send.at[0], recv_sem=z_recv.at[there],
            device_id=(y * 4 + there, b), device_id_type=MESH,
        ).wait_recv()
        joined = joined + from_z[there]
    summed[0 : 2 * H, :] = joined
    lanes = lax.broadcasted_iota(I32, (1, 128), 1)
    sign = jnp.where(lanes < 64, -1.0, 1.0).astype(F32)
    terms = three_terms(summed[...], 0)
    psi = turned(jnp.dot(factors[0:128, 0:144], terms, preferred_element_type=F32), sign)
    for p in range(BLKS):
        ps[p] = psi[2 * p : 2 * p + 2]

    def b_copy(i):
        there = members[i]
        return pltpu.make_async_remote_copy(
            src_ref=ps.at[there], dst_ref=got.at[b],
            send_sem=b_send.at[0], recv_sem=b_recv.at[b],
            device_id=(cycles, there), device_id_type=MESH,
        )

    b_copies = [b_copy(i) for i in range(BLKS - 1)]
    for copy in b_copies:
        copy.start()
    home = pltpu.make_async_remote_copy(
        src_ref=ps.at[b], dst_ref=got.at[b],
        send_sem=b_send.at[1], recv_sem=b_recv.at[b],
        device_id=(other, b), device_id_type=MESH,
    )

    @pl.when(turned_run)
    def _():
        home.start()

    @pl.when(zh != 2)
    def _():
        got[b] = ps[b]


    highs = lax.broadcasted_iota(I32, (32, 128), 0)
    for first in range(0, 16, 4):
        group = chips[first : first + 4]
        for source in [chip * 2 + c for chip in group for c in range(2)]:
            arrival = pltpu.make_async_remote_copy(
                src_ref=ps.at[0], dst_ref=got.at[source],
                send_sem=b_send.at[0], recv_sem=b_recv.at[source],
                device_id=(e, members[0]), device_id_type=MESH,
            )

            @pl.when((b != source) | turned_run)
            def _():
                arrival.wait_recv()

        parts = []
        for chip in group:
            for c in range(2):
                value = got[chip * 2 + c]
                here = highs == key[2 + c, chip : chip + 1, :]
                spread = jnp.concatenate(
                    [jnp.where(here, value[tt : tt + 1, :], 0.0) for tt in range(2)], axis=0
                )
                parts.append(jnp.concatenate(two_parts(spread), axis=0))
        placed = lax.dot_general(
            jnp.concatenate(parts, axis=1),
            jnp.concatenate([hot_low[chip] for chip in group], axis=1),
            (((1,), (1,)), ((), ())), preferred_element_type=F32,
        )
        grid[...] += placed[0:64] + placed[64:128]

    results = []
    for tt in range(2):
        terms = three_terms(grid[tt * 32 : tt * 32 + 32, :], 0)
        first = turned(jnp.dot(factors[128:256, 0:96], terms, preferred_element_type=F32), sign)
        results.append(three_terms(first * const[0:64, :] + rotated(first) * const[64:128, :], 1))
    last = lax.dot_general(
        factors[256:320, :], jnp.concatenate(results, axis=0), (((1,), (1,)), ((), ())),
        preferred_element_type=F32,
    )
    low, upp = last[0:32], last[32:64]
    left = lax.broadcasted_iota(I32, (32, 128), 1) < 64
    left_ref[0] = jnp.where(left, low, 0.0)
    right_ref[0] = jnp.where(left, 0.0, rotated(upp))
    left_ref[1] = jnp.where(left, rotated(low), 0.0)
    right_ref[1] = jnp.where(left, 0.0, upp)
    for copy in y_copies + z_copies:
        copy.wait_send()
    pltpu.make_async_remote_copy(
        src_ref=to_ell.at[0:15], dst_ref=from_ell.at[0:15], send_sem=e_send.at[0],
        recv_sem=e_recv.at[0], device_id=(owners[0], b), device_id_type=MESH,
    ).wait_send()
    pltpu.make_async_remote_copy(
        src_ref=ps.at[0 : BLKS - 1], dst_ref=got.at[0 : BLKS - 1], send_sem=b_send.at[0],
        recv_sem=b_recv.at[0], device_id=(e, members[0]), device_id_type=MESH,
    ).wait_send()

    @pl.when(turned_run)
    def _():
        home.wait_send()


def on_device(wigner, sky_alm, beam_blm, slot_col, slot_ell, order_of_column):
    q = wigner.shape[2]
    any_space = pl.BlockSpec(memory_space=pltpu.HBM)
    dma = pltpu.SemaphoreType.DMA
    left, right = pl.pallas_call(
        kernel,
        out_shape=[jax.ShapeDtypeStruct((2, 32, 128), F32)] * 2,
        in_specs=[any_space] * 8,
        out_specs=[pl.BlockSpec(memory_space=pltpu.VMEM)] * 2,
        scratch_shapes=[
            pltpu.VMEM((K, T, q), BF16),
            pltpu.VMEM((2, q), F32),
            pltpu.VMEM((K, 2, 2048), F32),
            pltpu.VMEM((q // 128, 128), I32),
            pltpu.VMEM((q // 128, 128), I32),
            pltpu.VMEM((16, 128), I32),
            pltpu.VMEM((128, 128), F32),
            pltpu.VMEM((320, 384), BF16),
            pltpu.VMEM((16, 40, 128), F32),
            pltpu.VMEM((2, 24, q), F32),
            pltpu.VMEM((K, T, 128), F32),
            pltpu.VMEM((16, K - H, 2, 128), F32),
            pltpu.VMEM((16, K - H, 2, 128), F32),
            pltpu.VMEM((4, H, 8, 128), F32),
            pltpu.VMEM((H * 8, 128), F32),
            pltpu.VMEM((4, 2 * H, 128), F32),
            pltpu.VMEM((4, 2 * H, 128), F32),
            pltpu.VMEM((48, 128), F32),
            pltpu.VMEM((BLKS, 2, 128), F32),
            pltpu.VMEM((BLKS, 2, 128), F32),
            pltpu.VMEM((4, 16, 128), I32),
            pltpu.VMEM((16, 128, 256), BF16),
            pltpu.VMEM((64, 128), F32),
            dma((8,)),
            dma((1,)), dma((16,)), dma((3,)), dma((4,)), dma((3,)), dma((4,)), dma((2,)), dma((BLKS,)),
        ],
        compiler_params=pltpu.CompilerParams(
            collective_id=0, has_side_effects=True, vmem_limit_bytes=40 * 1024 * 1024
        ),
    )(
        *(
            pltpu.with_memory_space_constraint(operand, pltpu.HBM)
            for operand in (
                jnp.transpose(wigner, (1, 0, 2)),
                sky_alm,
                jnp.transpose(beam_blm, (1, 0, 2)),
                slot_col.reshape(q // 128, 128),
                slot_ell.reshape(q // 128, 128),
                order_of_column.reshape(16, 128),
                *constants(),
            )
        )
    )
    return left.reshape(2, 1, 4096) + right.reshape(2, 1, 4096)


def solution(mesh):
    return jax.shard_map(
        on_device,
        mesh=mesh,
        in_specs=(
            P(None, None, ("ell", "blk")),
            P(None, ("ell", "blk")),
            P(),
            P(("ell", "blk")),
            P(("ell", "blk")),
            P(),
        ),
        out_specs=P("ell", "blk", None),
        check_vma=False,
    )
```
